32 devices in a mesh: row: 4 (over y, x), col: 4 (over z), depth: 2 (over core).
Axes of the slice: x: 2, y: 2, z: 4, core: 2. Of those that a mesh axis runs over, the one named last changes fastest.
Arguments:
- orbitals: bfloat16 [2, 1024, 2, 4096], P(None, ('row', 'col'), 'depth'), may hold values from -20 to 20
- potential: float32 [2, 4096], P('depth'), may hold values from -6 to 6
Outputs:
- intersection: float32 [1024, 2, 1024], P(('row', 'depth'), None, 'col')
- applied: bfloat16 [2, 1024, 2, 4096], P(None, ('row', 'col'), 'depth')
The draws below stay inside these ranges and needn't reach their ends.
All inputs are finite; a program needn't handle non-finite values.
Results may differ from the reference program's by a relative error of at most 0.001.
Values may be sent and summed in bfloat16 or wider, within the bound.
A program may use at most 128 MiB of HBM per device.

```python
import jax
import jax.numpy as jnp
from jax import lax

NORB = 1024
NX = 64
NZ = 2
NYX = 4096


def draw_orbitals(key, part):
    base_key = jax.random.fold_in(key, 11)
    first, second = jax.random.split(base_key, 2)
    shape = (2, NORB, NZ, NYX)
    noise = jnp.clip(jax.random.normal(first, shape, jnp.float32), -4.0, 4.0)
    scales = jnp.exp(jax.random.uniform(second, (1, NORB, 1, 1), jnp.float32, -0.69, 0.69))
    mixed = noise + 0.6 * jnp.roll(noise, 1, axis=1) + 0.4 * jnp.roll(noise, 37, axis=1)
    total = mixed * scales
    return jnp.clip(total, -20.0, 20.0).astype(jnp.bfloat16)


def block_levels(own_key, dims, shards, low, largest):
    def one(axis_at, shards_of):
        draws = jax.random.uniform(jax.random.fold_in(jax.random.fold_in(own_key, 6), axis_at), (shards_of,), jnp.float32, low / len(shards), largest / len(shards))
        return jnp.repeat(jnp.exp(draws), dims[axis_at] // shards_of).reshape((-1,) + (1,) * (len(dims) - axis_at - 1))

    gain = one(*shards[0])
    for cut in shards[1:]:
        gain = gain * one(*cut)
    return gain


def gaussian(own_key, dims, deviation, bound, cuts=(), dtype=jnp.bfloat16):
    level = block_levels(own_key, dims, cuts, -0.22, 0.18) if cuts else 1.0
    array = jax.random.normal(own_key, dims, jnp.float32) * deviation * level
    return jnp.minimum(jnp.maximum(array, -bound), bound).astype(dtype)


def setup_inputs(seed: int = 0) -> dict:
    arg_keys = jax.random.split(jax.random.key(seed), 3)
    return {
        "orbitals": draw_orbitals(jax.random.fold_in(arg_keys[2], 71), 0),
        "potential": gaussian(arg_keys[1], (NZ, NYX), 1.0, 6.0, ((0, 2),), jnp.float32),
    }


def apply_operator(field, potential):
    flat_cells = field.shape[-1]
    xpos = jnp.arange(flat_cells) % NX
    below = jnp.roll(field, 1, axis=2)
    above = jnp.roll(field, -1, axis=2)
    yminus = jnp.roll(field, NX, axis=3)
    yplus = jnp.roll(field, -NX, axis=3)
    xminus = jnp.where(xpos == 0, jnp.roll(field, 1 - NX, axis=3), jnp.roll(field, 1, axis=3))
    xplus = jnp.where(xpos == NX - 1, jnp.roll(field, NX - 1, axis=3), jnp.roll(field, -1, axis=3))
    lap = below + above + yminus + yplus + xminus + xplus - 6.0 * field
    return -0.5 * lap + potential[None, None] * field


def reference(orbitals, potential):
    wide = orbitals.astype(jnp.float32)
    cells = NZ * NYX
    real_part = wide[0].reshape(NORB, cells)
    imag_part = wide[1].reshape(NORB, cells)
    dvol = 1.0 / cells
    high = lax.Precision.HIGHEST
    sreal = jnp.dot(real_part, real_part.T, precision=high) + jnp.dot(imag_part, imag_part.T, precision=high)
    simag = jnp.dot(real_part, imag_part.T, precision=high) - jnp.dot(imag_part, real_part.T, precision=high)
    intersection = jnp.stack([sreal * dvol, simag * dvol], axis=1)
    applied = apply_operator(wide, potential).astype(jnp.bfloat16)
    return intersection, applied
```

```python
import functools

import jax
import jax.numpy as jnp
from jax import lax
from jax.experimental import pallas as pl
from jax.experimental.pallas import tpu as pltpu
from jax.sharding import PartitionSpec as P

NX = 64
MESH = pl.DeviceIdType.MESH


def with_halo(block, sides, width):
    for axis, dim in sides:
        count = lax.axis_size(axis)
        forward = [(i, i + 1) for i in range(count - 1)]
        forward.append((count - 1, 0))
        backward = [(target, source) for source, target in forward]
        low = lax.ppermute(
            lax.slice_in_dim(block, block.shape[dim] - width, None, axis=dim), axis, forward
        )
        high = lax.ppermute(lax.slice_in_dim(block, 0, width, axis=dim), axis, backward)
        block = jnp.concatenate([low, block, high], axis=dim)
    return block


def apply_operator(padded, potential):
    center = padded[:, :, 1:-1].astype(jnp.float32)
    below = padded[:, :, :-2].astype(jnp.float32)
    above = padded[:, :, 2:].astype(jnp.float32)
    flat_cells = center.shape[-1]
    xpos = jnp.arange(flat_cells) % NX
    yminus = jnp.roll(center, NX, axis=3)
    yplus = jnp.roll(center, -NX, axis=3)
    xminus = jnp.where(xpos == 0, jnp.roll(center, 1 - NX, axis=3), jnp.roll(center, 1, axis=3))
    xplus = jnp.where(
        xpos == NX - 1, jnp.roll(center, NX - 1, axis=3), jnp.roll(center, -1, axis=3)
    )
    lap = below + above + yminus + yplus + xminus + xplus - 6.0 * center
    return (-0.5 * lap + potential[None, None] * center).astype(jnp.bfloat16)


def contract(left, right):
    return lax.dot_general(
        left, right, (((1,), (1,)), ((), ())), preferred_element_type=jnp.float32
    )


def shards(orbitals, potential):
    parts, orbs, planes, cells = orbitals.shape
    flat = orbitals.reshape(parts, orbs, planes * cells)
    panel = lax.all_gather(flat, "col", axis=1, tiled=True)
    other = lax.all_gather(flat, "row", axis=1, tiled=True)
    padded = with_halo(orbitals, (("depth", 2),), 1)
    applied = apply_operator(padded, potential)
    dvol = 1.0 / (planes * lax.axis_size("depth") * cells)
    tile_cols = other.shape[1]
    real_rows = panel[0]
    imag_rows = panel[1]
    sreal = contract(real_rows, other[0]) + contract(imag_rows, other[1])
    simag = contract(real_rows, other[1]) - contract(imag_rows, other[0])
    summed = lax.psum_scatter(
        dvol * jnp.concatenate([sreal, simag], axis=1), "depth", scatter_dimension=0, tiled=True
    )
    intersection = summed.reshape(summed.shape[0], 2, tile_cols)
    intersection = lax.all_to_all(intersection, "col", split_axis=2, concat_axis=2, tiled=True)
    return (intersection, applied)


def flip(a, b):
    low = lax.rem(lax.rem(a, 2) + lax.rem(b, 2), 2)
    high = lax.rem(lax.div(a, 2) + lax.div(b, 2), 2)
    return 2 * high + low


def stencil(orb, halo, pot, out):
    parts, orbs, cells = orb.shape
    step = 16
    xpos = lax.broadcasted_iota(jnp.int32, (step, cells), 1) % NX
    first, last = xpos == 0, xpos == NX - 1

    def body(i, carry):
        part = lax.div(i, orbs // step)
        rows = pl.ds(pl.multiple_of(lax.rem(i, orbs // step) * step, step), step)
        center = orb[part, rows, :].astype(jnp.float32)
        side = halo[part, rows, :].astype(jnp.float32)
        right = pltpu.roll(center, 1, 1)
        left = pltpu.roll(center, cells - 1, 1)
        yminus = pltpu.roll(center, NX, 1)
        yplus = pltpu.roll(center, cells - NX, 1)
        xminus = jnp.where(first, pltpu.roll(right, cells - NX, 1), right)
        xplus = jnp.where(last, pltpu.roll(left, NX, 1), left)
        lap = side + side + yminus + yplus + xminus + xplus - 6.0 * center
        out[part, rows, :] = (-0.5 * lap + pot[0:1, :] * center).astype(out.dtype)
        return carry

    lax.fori_loop(0, parts * (orbs // step), body, 0)


STAGES = ((0, 2), (2, 3), (3, 4))
PIECES = ((0, 0, 4), (1, 0, 5), (2, 0, 4), (2, 4, 3))
GROUPS = 4
OUTER, INNER = 0, 1
MEMBERS = (
    ((OUTER, 0), (OUTER, 1)),
    ((OUTER, 2), (INNER, 0)),
    ((OUTER, 3), (INNER, 1)),
    ((INNER, 2), (INNER, 3)),
)
PLACE = {member: (g, u) for g, pair in enumerate(MEMBERS) for u, member in enumerate(pair)}


def blocks():
    order, spans = {}, []
    for low, high in STAGES:
        begin = len(order)
        for a in range(high):
            for b in range(high):
                if max(a, b) >= low:
                    order[a, b] = len(order)
        spans.append((begin, len(order) - begin))
    return order, spans


def kernel(dvol, orb_hbm, pot_hbm, inter, applied, orb, pot, halo, panel, acc, take, pacc, ptake,
           land, relay, ins, hs, hr, ls, zs, zr, xs, xr, ds, dr, gs, gr, qr, rs, rr):
    r, c, d = lax.axis_index("row"), lax.axis_index("col"), lax.axis_index("depth")
    parts, orbs, cells = orb.shape
    quarter = cells // 4
    size = orbs // GROUPS
    wide = 8 * size
    order, spans = blocks()
    load = pltpu.make_async_copy(orb_hbm, orb, ins.at[0])
    load.start()
    load_pot = pltpu.make_async_copy(pot_hbm, pot, ins.at[1])
    load_pot.start()
    peer = (r, c, 1 - d)
    zdev = [None] + [(r, flip(c, k), d) for k in (1, 2, 3)]
    xdev = [None] + [(flip(r, k), c, d) for k in (1, 2)]

    barrier = pltpu.get_barrier_semaphore()
    friends = [peer] + zdev[1:] + xdev[1:]
    for dev in friends:
        pl.semaphore_signal(barrier, inc=1, device_id=dev, device_id_type=MESH)
    load.wait()
    pl.semaphore_wait(barrier, len(friends))

    def send(src, dst, ssem, rsem, dev):
        return pltpu.make_async_remote_copy(
            src_ref=src, dst_ref=dst, send_sem=ssem, recv_sem=rsem,
            device_id=dev, device_id_type=MESH,
        )

    def own(g, k):
        lanes = pl.ds(pl.multiple_of(k * quarter, quarter), quarter)
        return orb.at[:, pl.ds(g * size, size), lanes]

    def spot(j, m, k):
        deep = lax.rem(k + 1, 4) >= 2
        g, u = (jnp.where(deep, i, o) for i, o in zip(PLACE[INNER, m], PLACE[OUTER, m]))
        return panel.at[j, g, :, u, lax.div(k, 2)]

    def go(cp):
        cp.start()
        return cp

    def flush(ref, sem):
        pltpu.make_async_copy(ref, ref, sem).wait()

    zsend, xsend, pair, cross = {}, {}, {}, {}
    for g in range(GROUPS):
        for k in (1, 3, 2):
            zsend[k, g] = go(send(own(g, flip(c, k)), spot(0, g, c), zs, zr.at[k, g], zdev[k]))
    for g in range(GROUPS):
        for j in (1, 2):
            xsend[0, j, g] = go(send(own(g, c), spot(j, g, c), xs, xr.at[0, j, g], xdev[j]))
    edge = send(orb, halo, hs, hr, peer)
    edge.start()
    local = [pltpu.make_async_copy(own(g, c), spot(0, g, c), ls.at[g]) for g in range(GROUPS)]
    for cp in local:
        cp.start()

    inner = lax.rem(c + 1, 4) >= 2
    lane = lax.broadcasted_iota(jnp.int32, (1, 2 * wide // 2), 1)
    sign = jnp.where(lane < wide // 2, 1.0, -1.0).astype(jnp.float32)

    def fold(x):
        rows = x.shape[0] // 2
        return x[:rows] + sign * pltpu.roll(x[rows:], wide // 2, 1)

    def span(s):
        begin, count = spans[s]
        return pl.ds(begin, count)

    def forward(k, g):
        zsend[k, g].wait_recv()
        for j in (1, 2):
            part = spot(0, g, flip(c, k)), spot(j, g, flip(c, k))
            send(*part, xs, xr.at[k, j, g], xdev[j]).start()

    def forwards(deep, shallow):
        @pl.when(inner)
        def _():
            for k, m in deep:
                forward(k, m)

        @pl.when(jnp.logical_not(inner))
        def _():
            for k, m in shallow:
                forward(k, m)

    def arrived(k, m):
        for j in (1, 2):
            src, dst = spot(0, m, flip(c, k)), spot(j, m, flip(c, k))
            send(src, dst, xs, xr.at[k, j, m], xdev[j]).wait_recv()

    def gathered(g):
        for kind, m in MEMBERS[g]:
            same = inner if kind == INNER else jnp.logical_not(inner)

            @pl.when(same)
            def _():
                arrived(0, m)
                arrived(3, m)

            @pl.when(jnp.logical_not(same))
            def _():
                arrived(1, m)
                arrived(2, m)

    def fresh(s):
        return [(a, b) for a, b in order if spans[s][0] <= order[a, b] < sum(spans[s])]

    def tile(t, s):
        top = STAGES[s][1]
        left = panel[0, 0:top].reshape(top * wide, quarter)
        right = panel[t, 0:top].reshape(top * wide, quarter)
        prod = contract(left, right)
        for a, b in fresh(s):
            x = fold(prod[a * wide:(a + 1) * wide, b * wide:(b + 1) * wide])
            x = x.reshape(2, 2, size, wide)
            for h in (0, 1):
                acc[t, h, order[a, b]] = x[:, h].reshape(2 * size, wide)
        pair[t, s] = go(send(acc.at[t, 1 - d, span(s)], take.at[t, span(s)], ds, dr.at[t, s], peer))

    def shared(s):
        top, half = STAGES[s][1], wide // 2
        for j in (1, 2):
            left = panel[j, 0:top, :, j - 1].reshape(top * half, quarter)
            right = panel[3 - j, 0:top].reshape(top * wide, quarter)
            prod = contract(left, right)
            for a, b in fresh(s):
                x = fold(prod[a * half:(a + 1) * half, b * wide:(b + 1) * wide])
                for h in (0, 1):
                    pacc[h, j - 1, order[a, b]] = x[h * size:(h + 1) * size]
        pair[4, s] = go(send(pacc.at[1 - d, :, span(s)], ptake.at[:, span(s)], ds, dr.at[3, s], peer))

    def settle(t, s):
        pair[t, s].wait_recv()
        acc[t, d, span(s)] += take[t, span(s)]

    def swap(s):
        pair[4, s].wait_recv()
        pacc[d, :, span(s)] += ptake[:, span(s)]
        for j in (1, 2):
            dst = acc.at[3, d, span(s), pl.ds((j - 1) * size, size)]
            cross[j, s] = go(send(pacc.at[d, j - 1, span(s)], dst, rs, rr.at[j - 1, s], xdev[j]))

    def swapped(s):
        for j in (1, 2):
            cross[j, s].wait_recv()

    def route(t):
        to = flip(r, jnp.int32(t))
        return to, lax.div(to, 2) != lax.div(c, 2)

    def chunk(n):
        s, skip, count = PIECES[n]
        return pl.ds(spans[s][0] + skip, count)

    def far(t, s):
        to, across = route(t)

        @pl.when(jnp.logical_and(across, jnp.logical_not(inner)))
        def _():
            for n in range(len(PIECES)):
                if PIECES[n][0] == s:
                    send(acc.at[t, d, chunk(n)], relay.at[t, chunk(n)], gs, qr.at[t, n], zdev[1]).start()

    def near(t, s):
        to, across = route(t)

        @pl.when(jnp.logical_and(to != c, jnp.logical_not(across)))
        def _():
            send(acc.at[t, d, span(s)], land.at[0, span(s)], gs, gr.at[0, s], zdev[1]).start()

    def pass_on(t, n):
        to, across = route(t)

        @pl.when(jnp.logical_and(across, inner))
        def _():
            send(acc.at[t, d, chunk(n)], relay.at[t, chunk(n)], gs, qr.at[t, n], zdev[1]).wait_recv()
            acc[t, d, chunk(n)] += relay[t, chunk(n)]
            send(acc.at[t, d, chunk(n)], land.at[1, chunk(n)], gs, gr.at[1, n], (r, to, d)).start()

    def operator():
        load_pot.wait()
        edge.wait()
        stencil(orb, halo, pot, applied)
        for cp in local:
            cp.wait()

    operator()
    forwards(((1, 0), (3, 0), (2, 0), (1, 1), (2, 1), (1, 2), (2, 2)), ((1, 0), (3, 0), (2, 0), (3, 1), (1, 1), (3, 2)))
    tile(0, 0)
    forwards(((1, 3), (2, 3)), ((1, 2), (1, 3)))
    settle(0, 0)
    far(0, 0)
    near(0, 0)
    gathered(0)
    gathered(1)
    shared(0)
    forwards((), ((3, 3),))
    tile(2, 0)
    forwards(((3, 1),), ((2, 1),))
    tile(1, 0)
    swap(0)
    settle(2, 0)
    far(2, 0)
    settle(1, 0)
    far(1, 0)
    near(2, 0)
    near(1, 0)
    tile(0, 1)
    forwards(((3, 2),), ((2, 2),))
    settle(0, 1)
    far(0, 1)
    near(0, 1)
    gathered(2)
    shared(1)
    forwards(((3, 3),), ((2, 3),))
    tile(2, 1)
    tile(1, 1)
    swapped(0)
    far(3, 0)
    near(3, 0)
    tile(0, 2)
    swap(1)
    settle(2, 1)
    far(2, 1)
    settle(1, 1)
    far(1, 1)
    near(2, 1)
    near(1, 1)
    for t in (0, 2, 1, 3):
        pass_on(t, 0)
    pass_on(0, 1)
    gathered(3)
    shared(2)
    tile(2, 2)
    tile(1, 2)
    settle(0, 2)
    far(0, 2)
    swapped(1)
    far(3, 1)
    near(3, 1)
    swap(2)
    settle(2, 2)
    far(2, 2)
    settle(1, 2)
    far(1, 2)
    near(2, 2)
    for t in (2, 1, 3):
        pass_on(t, 1)
    pass_on(0, 2)
    pass_on(0, 3)
    swapped(2)
    far(3, 2)
    near(3, 2)
    near(0, 2)
    near(1, 2)
    pass_on(2, 2)
    pass_on(1, 2)
    pass_on(2, 3)
    pass_on(1, 3)
    pass_on(3, 2)
    pass_on(3, 3)

    flush(panel.at[0, 0:3], zs)
    flush(panel.at[0:2], xs)
    flush(acc.at[0:2], ds)
    flush(acc.at[0, 0], rs)
    mine = flip(r, c)
    for s in range(len(STAGES)):
        send(acc.at[0, d, span(s)], land.at[0, span(s)], gs, gr.at[0, s], zdev[1]).wait_recv()
    for n in range(len(PIECES)):
        send(acc.at[0, d, chunk(n)], land.at[1, chunk(n)], gs, gr.at[1, n], zdev[1]).wait_recv()
    half, quad = wide // 2, wide // 8
    pick = lax.div(lane, quad)
    for a in range(GROUPS):
        for u, (kind, m) in enumerate(MEMBERS[a]):
            total = []
            for b in range(GROUPS):
                i, rows = order[a, b], pl.ds(u * size, size)
                total.append((acc[mine, d, i, rows] + land[0, i, rows] + land[1, i, rows]) * dvol)
            first = (d if kind == OUTER else 1 - d) * half + m * size
            for part in range(parts):
                for v in (0, 1):
                    out = None
                    for b in range(GROUPS):
                        for w, (col, n) in enumerate(MEMBERS[b]):
                            at = part * half + w * 2 * quad + v * quad
                            to = (col ^ v) * half + n * quad
                            moved = pltpu.roll(total[b], (to - at) % wide, 1)
                            out = moved if out is None else jnp.where(pick == to // quad, moved, out)
                    rows = pl.ds(pl.multiple_of(first, size), size)
                    inter[part, rows, pl.ds(v * wide, wide)] = out

    flush(relay.at[0:3], gs)


def exchange(orbitals, potential):
    parts, orbs, planes, cells = orbitals.shape
    rows = orbs * lax.axis_size("col")
    half = rows // 2
    size = orbs // GROUPS
    count = GROUPS * GROUPS
    steps, pieces = len(STAGES), len(PIECES)
    dvol = 1.0 / (planes * lax.axis_size("depth") * cells)
    vmem = pl.BlockSpec(memory_space=pltpu.VMEM)
    dma = pltpu.SemaphoreType.DMA
    block = (count, 2 * size, 8 * size)
    inter, applied = pl.pallas_call(
        functools.partial(kernel, dvol),
        out_shape=(
            jax.ShapeDtypeStruct((2, half, rows), jnp.float32),
            jax.ShapeDtypeStruct((parts, orbs, cells), jnp.bfloat16),
        ),
        in_specs=[pl.BlockSpec(memory_space=pltpu.HBM)] * 2,
        out_specs=(vmem, vmem),
        scratch_shapes=[
            pltpu.VMEM((parts, orbs, cells), jnp.bfloat16),
            pltpu.VMEM(potential.shape, jnp.float32),
            pltpu.VMEM((parts, orbs, cells), jnp.bfloat16),
            pltpu.VMEM((3, GROUPS, parts, 2, 2, size, cells // 4), jnp.bfloat16),
            pltpu.VMEM((4, 2) + block, jnp.float32),
            pltpu.VMEM((3,) + block, jnp.float32),
            pltpu.VMEM((2, 2, count, size, 8 * size), jnp.float32),
            pltpu.VMEM((2, count, size, 8 * size), jnp.float32),
            pltpu.VMEM((2,) + block, jnp.float32),
            pltpu.VMEM((4,) + block, jnp.float32),
            dma((2,)), dma, dma, dma((GROUPS,)), dma, dma((4, GROUPS)), dma,
            dma((4, 3, GROUPS)), dma, dma((4, steps)), dma, dma((2, pieces)),
            dma((4, pieces)), dma, dma((2, steps)),
        ],
        compiler_params=pltpu.CompilerParams(
            collective_id=0, has_side_effects=True, vmem_limit_bytes=55000000
        ),
        name="overlap",
    )(orbitals.reshape(parts, orbs, cells), potential)
    return jnp.transpose(inter, (1, 0, 2)), applied.reshape(orbitals.shape)


def solution(mesh):
    in_specs = (P(None, ("row", "col"), "depth", None), P("depth", None))
    out_specs = (P(("row", "depth"), None, "col"), P(None, ("row", "col"), "depth", None))
    sizes = tuple(mesh.shape[axis] for axis in ("row", "col", "depth"))
    body = exchange if sizes == (4, 4, 2) else shards
    return jax.shard_map(body, mesh=mesh, in_specs=in_specs, out_specs=out_specs, check_vma=False)
```

```python
import functools

import jax
import jax.numpy as jnp
from jax import lax
from jax.experimental import pallas as pl
from jax.experimental.pallas import tpu as pltpu
from jax.sharding import PartitionSpec as P

NX = 64
MESH = pl.DeviceIdType.MESH


def with_halo(block, sides, width):
    for axis, dim in sides:
        count = lax.axis_size(axis)
        forward = [(i, i + 1) for i in range(count - 1)]
        forward.append((count - 1, 0))
        backward = [(target, source) for source, target in forward]
        low = lax.ppermute(
            lax.slice_in_dim(block, block.shape[dim] - width, None, axis=dim), axis, forward
        )
        high = lax.ppermute(lax.slice_in_dim(block, 0, width, axis=dim), axis, backward)
        block = jnp.concatenate([low, block, high], axis=dim)
    return block


def apply_operator(padded, potential):
    center = padded[:, :, 1:-1].astype(jnp.float32)
    below = padded[:, :, :-2].astype(jnp.float32)
    above = padded[:, :, 2:].astype(jnp.float32)
    flat_cells = center.shape[-1]
    xpos = jnp.arange(flat_cells) % NX
    yminus = jnp.roll(center, NX, axis=3)
    yplus = jnp.roll(center, -NX, axis=3)
    xminus = jnp.where(xpos == 0, jnp.roll(center, 1 - NX, axis=3), jnp.roll(center, 1, axis=3))
    xplus = jnp.where(
        xpos == NX - 1, jnp.roll(center, NX - 1, axis=3), jnp.roll(center, -1, axis=3)
    )
    lap = below + above + yminus + yplus + xminus + xplus - 6.0 * center
    return (-0.5 * lap + potential[None, None] * center).astype(jnp.bfloat16)


def contract(left, right):
    return lax.dot_general(
        left, right, (((1,), (1,)), ((), ())), preferred_element_type=jnp.float32
    )


def shards(orbitals, potential):
    parts, orbs, planes, cells = orbitals.shape
    flat = orbitals.reshape(parts, orbs, planes * cells)
    panel = lax.all_gather(flat, "col", axis=1, tiled=True)
    other = lax.all_gather(flat, "row", axis=1, tiled=True)
    padded = with_halo(orbitals, (("depth", 2),), 1)
    applied = apply_operator(padded, potential)
    dvol = 1.0 / (planes * lax.axis_size("depth") * cells)
    tile_cols = other.shape[1]
    real_rows = panel[0]
    imag_rows = panel[1]
    sreal = contract(real_rows, other[0]) + contract(imag_rows, other[1])
    simag = contract(real_rows, other[1]) - contract(imag_rows, other[0])
    summed = lax.psum_scatter(
        dvol * jnp.concatenate([sreal, simag], axis=1), "depth", scatter_dimension=0, tiled=True
    )
    intersection = summed.reshape(summed.shape[0], 2, tile_cols)
    intersection = lax.all_to_all(intersection, "col", split_axis=2, concat_axis=2, tiled=True)
    return (intersection, applied)


def flip(a, b):
    low = lax.rem(lax.rem(a, 2) + lax.rem(b, 2), 2)
    high = lax.rem(lax.div(a, 2) + lax.div(b, 2), 2)
    return 2 * high + low


def stencil(orb, halo, pot, out):
    parts, orbs, cells = orb.shape
    step = 16
    xpos = lax.broadcasted_iota(jnp.int32, (step, cells), 1) % NX
    first, last = xpos == 0, xpos == NX - 1

    def body(i, carry):
        part = lax.div(i, orbs // step)
        rows = pl.ds(pl.multiple_of(lax.rem(i, orbs // step) * step, step), step)
        center = orb[part, rows, :].astype(jnp.float32)
        side = halo[part, rows, :].astype(jnp.float32)
        right = pltpu.roll(center, 1, 1)
        left = pltpu.roll(center, cells - 1, 1)
        yminus = pltpu.roll(center, NX, 1)
        yplus = pltpu.roll(center, cells - NX, 1)
        xminus = jnp.where(first, pltpu.roll(right, cells - NX, 1), right)
        xplus = jnp.where(last, pltpu.roll(left, NX, 1), left)
        lap = side + side + yminus + yplus + xminus + xplus - 6.0 * center
        out[part, rows, :] = (-0.5 * lap + pot[0:1, :] * center).astype(out.dtype)
        return carry

    lax.fori_loop(0, parts * (orbs // step), body, 0)


STAGES = ((0, 2), (2, 3), (3, 4))
PIECES = ((0, 0, 4), (1, 0, 5), (2, 0, 4), (2, 4, 3))
GROUPS = 4
OUTER, INNER = 0, 1
MEMBERS = (
    ((OUTER, 0), (OUTER, 1)),
    ((OUTER, 2), (INNER, 0)),
    ((OUTER, 3), (INNER, 1)),
    ((INNER, 2), (INNER, 3)),
)
PLACE = {member: (g, u) for g, pair in enumerate(MEMBERS) for u, member in enumerate(pair)}


def blocks():
    order, spans = {}, []
    for low, high in STAGES:
        begin = len(order)
        for a in range(high):
            for b in range(high):
                if max(a, b) >= low:
                    order[a, b] = len(order)
        spans.append((begin, len(order) - begin))
    return order, spans


def kernel(dvol, orb_hbm, pot_hbm, inter, applied, orb, pot, halo, panel, acc, take, pacc, cross,
           land, relay, ptake, wire, ins, hs, hr, ls, zs, zr, xs, xr, ds, dr, gs, gr, qr, rs, rr, ps, pr, fs, fr):
    r, c, d = lax.axis_index("row"), lax.axis_index("col"), lax.axis_index("depth")
    parts, orbs, cells = orb.shape
    quarter = cells // 4
    size = orbs // GROUPS
    wide = 8 * size
    order, spans = blocks()
    load = pltpu.make_async_copy(orb_hbm, orb, ins.at[0])
    load.start()
    load_pot = pltpu.make_async_copy(pot_hbm, pot, ins.at[1])
    load_pot.start()
    peer = (r, c, 1 - d)
    zdev = [None] + [(r, flip(c, k), d) for k in (1, 2, 3)]
    xdev = [None] + [(flip(r, k), c, d) for k in (1, 2)]

    barrier = pltpu.get_barrier_semaphore()
    friends = [peer] + zdev[1:] + xdev[1:] + [(flip(r, k), c, 1 - d) for k in (1, 2)]
    for dev in friends:
        pl.semaphore_signal(barrier, inc=1, device_id=dev, device_id_type=MESH)
    load.wait()
    pl.semaphore_wait(barrier, len(friends))

    def send(src, dst, ssem, rsem, dev):
        return pltpu.make_async_remote_copy(
            src_ref=src, dst_ref=dst, send_sem=ssem, recv_sem=rsem,
            device_id=dev, device_id_type=MESH,
        )

    def own(g, k):
        lanes = pl.ds(pl.multiple_of(k * quarter, quarter), quarter)
        return orb.at[:, pl.ds(g * size, size), lanes]

    def place(m, k):
        deep = lax.rem(k + 1, 4) >= 2
        return [jnp.where(deep, i, o) for i, o in zip(PLACE[INNER, m], PLACE[OUTER, m])]

    def home(m, k):
        return place(m, k)[0]

    def spot(j, m, k):
        g, u = place(m, k)
        return panel.at[j, g, :, u, lax.div(k, 2)]

    def go(cp):
        cp.start()
        return cp

    def flush(ref, sem):
        pltpu.make_async_copy(ref, ref, sem).wait()

    zsend, pair = {}, {}
    for g in range(GROUPS):
        for k in (1, 3, 2):
            zsend[k, g] = go(send(own(g, flip(c, k)), spot(0, g, c), zs, zr.at[k, g], zdev[k]))
    for g in range(GROUPS):
        for j in (1, 2):
            send(own(g, c), spot(j, g, c), xs, xr.at[home(g, c)], xdev[j]).start()
    edge = send(orb, halo, hs, hr, peer)
    edge.start()
    for g in range(GROUPS):
        pltpu.make_async_copy(own(g, c), spot(0, g, c), ls).start()

    inner = lax.rem(c + 1, 4) >= 2
    lane = lax.broadcasted_iota(jnp.int32, (1, 2 * wide // 2), 1)
    sign = jnp.where(lane < wide // 2, 1.0, -1.0).astype(jnp.float32)

    def fold(x):
        rows = x.shape[0] // 2
        return x[:rows] + sign * pltpu.roll(x[rows:], wide // 2, 1)

    def span(s):
        begin, count = spans[s]
        return pl.ds(begin, count)

    def forward(k, g):
        zsend[k, g].wait_recv()
        for j in (1, 2):
            part = spot(0, g, flip(c, k)), spot(j, g, flip(c, k))
            send(*part, xs, xr.at[home(g, flip(c, k))], xdev[j]).start()

    def forwards(deep, shallow):
        @pl.when(inner)
        def _():
            for k, m in deep:
                forward(k, m)

        @pl.when(jnp.logical_not(inner))
        def _():
            for k, m in shallow:
                forward(k, m)

    last = len(STAGES) - 1

    def gathered(g):
        flush(panel.at[1:3, g], xr.at[g])

    def fresh(s):
        return [(a, b) for a, b in order if spans[s][0] <= order[a, b] < sum(spans[s])]

    def tile(t, s):
        top = STAGES[s][1]
        left = panel[0, 0:top].reshape(top * wide, quarter)
        right = panel[t, 0:top].reshape(top * wide, quarter)
        prod = contract(left, right)
        for a, b in fresh(s):
            x = fold(prod[a * wide:(a + 1) * wide, b * wide:(b + 1) * wide])
            x = x.reshape(2, 2, size, wide)
            for h in (0, 1):
                acc[t, h, order[a, b]] = x[:, h].reshape(2 * size, wide)
        pair[t, s] = go(send(acc.at[t, 1 - d, span(s)], take.at[t, span(s)], ds, dr.at[t, s], peer))

    def shared(s):
        top, half = STAGES[s][1], wide // 2
        for j in (1, 2):
            left = panel[j, 0:top, :, j - 1].reshape(top * half, quarter)
            right = panel[3 - j, 0:top].reshape(top * wide, quarter)
            prod = contract(left, right)
            for a, b in fresh(s):
                x = fold(prod[a * half:(a + 1) * half, b * wide:(b + 1) * wide])
                for h in (0, 1):
                    pacc[h, j - 1, order[a, b]] = x[h * size:(h + 1) * size]
            if s == last:
                for h in (0, 1):
                    dev = (flip(r, jnp.int32(j)), c, jnp.int32(h))
                    send(pacc.at[h, j - 1, span(s)], cross.at[j - 1, d], fs, fr, dev).start()
        if s < last:
            send(pacc.at[1 - d, :, span(s)], ptake.at[:, span(s)], ps, pr.at[s], peer).start()

    def settle(t, s):
        pair[t, s].wait_recv()
        acc[t, d, span(s)] += take[t, span(s)]

    def swap(s):
        flush(ptake.at[:, span(s)], pr.at[s])
        pacc[d, :, span(s)] += ptake[:, span(s)]
        for j in (1, 2):
            dst = acc.at[3, d, span(s), pl.ds((j - 1) * size, size)]
            send(pacc.at[d, j - 1, span(s)], dst, rs, rr.at[s], xdev[j]).start()

    def swapped(s):
        if s < last:
            flush(acc.at[3, d, span(s)], rr.at[s])
        else:
            flush(cross, fr)
            for j in (0, 1):
                acc[3, d, span(s), pl.ds(j * size, size)] = cross[j, 0] + cross[j, 1]

    def encode(t, blocks):
        x = acc[t, d, blocks]
        high = x.astype(jnp.bfloat16)
        base = high.astype(jnp.float32)
        steps = jnp.round((x - base) / jnp.maximum(jnp.abs(base), 1e-37) * 2048.0)
        steps = jnp.clip(steps, -7.0, 7.0)
        wire[t, blocks, :2 * size] = high
        wire[t, blocks, 2 * size:] = (steps[:, :size] * 16.0 + steps[:, size:]).astype(jnp.bfloat16)

    def decode(words):
        base = words[:, :2 * size].astype(jnp.float32)
        code = words[:, 2 * size:].astype(jnp.float32)
        first = jnp.round(code / 16.0)
        steps = jnp.concatenate([first, code - 16.0 * first], axis=1)
        return base + steps * jnp.abs(base) / 2048.0

    def route(t):
        to = flip(r, jnp.int32(t))
        return to, lax.div(to, 2) != lax.div(c, 2)

    def chunk(n):
        s, skip, count = PIECES[n]
        return pl.ds(spans[s][0] + skip, count)

    def far(t, s):
        to, across = route(t)

        @pl.when(jnp.logical_and(across, jnp.logical_not(inner)))
        def _():
            for n in range(len(PIECES)):
                if PIECES[n][0] == s:
                    encode(t, chunk(n))
                    send(wire.at[t, chunk(n)], relay.at[t, chunk(n)], gs, qr.at[t, n], zdev[1]).start()

    def near(t, s, side):
        to, across = route(t)

        @pl.when(jnp.logical_and(jnp.logical_and(to != c, jnp.logical_not(across)), side))
        def _():
            encode(t, span(s))
            send(wire.at[t, span(s)], land.at[0, span(s)], gs, gr, zdev[1]).start()

    def pass_on(t, n):
        to, across = route(t)

        @pl.when(jnp.logical_and(across, inner))
        def _():
            flush(relay.at[t, chunk(n)], qr.at[t, n])
            acc[t, d, chunk(n)] += decode(relay[t, chunk(n)])
            encode(t, chunk(n))
            send(wire.at[t, chunk(n)], land.at[1, chunk(n)], gs, gr, (r, to, d)).start()

    deep, edge_chip = inner, jnp.logical_not(inner)

    def operator():
        load_pot.wait()
        edge.wait()
        stencil(orb, halo, pot, applied)
        flush(panel.at[0, 0], ls)

    operator()
    forwards(((1, 0), (3, 0), (2, 0), (1, 1), (2, 1), (1, 2), (2, 2)), ((1, 0), (3, 0), (2, 0), (3, 1), (1, 1), (3, 2)))
    tile(0, 0)
    forwards(((1, 3), (2, 3)), ((1, 2), (1, 3)))
    settle(0, 0)
    far(0, 0)
    near(0, 0, True)
    gathered(0)
    gathered(1)
    shared(0)
    forwards((), ((3, 3),))
    tile(2, 0)
    forwards(((3, 1),), ((2, 1),))
    tile(1, 0)
    swap(0)
    settle(2, 0)
    far(2, 0)
    settle(1, 0)
    far(1, 0)
    near(2, 0, True)
    near(1, 0, True)
    tile(0, 1)
    forwards(((3, 2),), ((2, 2),))
    settle(0, 1)
    far(0, 1)
    near(0, 1, True)
    swapped(0)
    far(3, 0)
    near(3, 0, True)
    gathered(2)
    forwards(((3, 3),), ((2, 3),))
    shared(1)
    pass_on(0, 0)
    pass_on(2, 0)
    tile(2, 1)
    pass_on(1, 0)
    tile(1, 1)
    swap(1)
    settle(2, 1)
    far(2, 1)
    pass_on(0, 1)
    tile(0, 2)
    settle(1, 1)
    far(1, 1)
    near(2, 1, True)
    near(1, 1, True)
    pass_on(3, 0)
    gathered(3)
    shared(2)
    tile(2, 2)
    settle(0, 2)
    far(0, 2)
    near(0, 2, deep)
    swapped(1)
    far(3, 1)
    near(3, 1, deep)
    pass_on(2, 1)
    tile(1, 2)
    pass_on(1, 1)
    settle(2, 2)
    far(2, 2)
    near(2, 2, deep)
    settle(1, 2)
    far(1, 2)
    near(1, 2, deep)
    near(3, 1, edge_chip)
    near(2, 2, edge_chip)
    pass_on(0, 2)
    pass_on(0, 3)
    swapped(2)
    far(3, 2)
    near(3, 2, True)
    near(0, 2, edge_chip)
    near(1, 2, edge_chip)
    pass_on(3, 1)
    pass_on(2, 2)
    pass_on(1, 2)
    pass_on(2, 3)
    pass_on(1, 3)
    pass_on(3, 2)
    pass_on(3, 3)

    flush(panel.at[0, 0:3], zs)
    flush(panel.at[0:2], xs)
    flush(take, ds)
    flush(acc.at[3, 0, 0:spans[last][0]], rs)
    flush(ptake, ps)
    flush(cross, fs)
    mine = flip(r, c)
    flush(land, gr)
    acc[mine, d] = (acc[mine, d] + decode(land[0]) + decode(land[1])) * dvol
    half, quad = wide // 2, wide // 8
    pick = lax.div(lane, quad)
    for a in range(GROUPS):
        for u, (kind, m) in enumerate(MEMBERS[a]):
            total = []
            for b in range(GROUPS):
                i, rows = order[a, b], pl.ds(u * size, size)
                total.append(acc[mine, d, i, rows])
            first = (d if kind == OUTER else 1 - d) * half + m * size
            for part in range(parts):
                for v in (0, 1):
                    out = None
                    for b in range(GROUPS):
                        for w, (col, n) in enumerate(MEMBERS[b]):
                            at = part * half + w * 2 * quad + v * quad
                            to = (col ^ v) * half + n * quad
                            moved = pltpu.roll(total[b], (to - at) % wide, 1)
                            out = moved if out is None else jnp.where(pick == to // quad, moved, out)
                    rows = pl.ds(pl.multiple_of(first, size), size)
                    inter[part, rows, pl.ds(v * wide, wide)] = out

    flush(relay.at[0:3], gs)


def publish(inter, applied, inter_out, applied_out, mixed, sems):
    whole = pltpu.make_async_copy(applied, applied_out, sems.at[0])
    whole.start()
    for part in (0, 1):
        mixed[:, part, :] = inter[part]
    tiles = pltpu.make_async_copy(mixed, inter_out, sems.at[1])
    tiles.start()
    whole.wait()
    tiles.wait()


def stay(array):
    return pltpu.with_memory_space_constraint(array, pltpu.HBM)


def exchange(orbitals, potential):
    parts, orbs, planes, cells = orbitals.shape
    rows = orbs * lax.axis_size("col")
    half = rows // 2
    size = orbs // GROUPS
    count = GROUPS * GROUPS
    steps, pieces = len(STAGES), len(PIECES)
    dvol = 1.0 / (planes * lax.axis_size("depth") * cells)
    vmem = pl.BlockSpec(memory_space=pltpu.VMEM)
    dma = pltpu.SemaphoreType.DMA
    block = (count, 2 * size, 8 * size)
    early = blocks()[1][-1][0]
    inter, applied = pl.pallas_call(
        functools.partial(kernel, dvol),
        out_shape=(
            jax.ShapeDtypeStruct((2, half, rows), jnp.float32),
            jax.ShapeDtypeStruct((parts, orbs, cells), jnp.bfloat16),
        ),
        in_specs=[pl.BlockSpec(memory_space=pltpu.HBM)] * 2,
        out_specs=(vmem, vmem),
        scratch_shapes=[
            pltpu.VMEM((parts, orbs, cells), jnp.bfloat16),
            pltpu.VMEM(potential.shape, jnp.float32),
            pltpu.VMEM((parts, orbs, cells), jnp.bfloat16),
            pltpu.VMEM((3, GROUPS, parts, 2, 2, size, cells // 4), jnp.bfloat16),
            pltpu.VMEM((4, 2) + block, jnp.float32),
            pltpu.VMEM((3,) + block, jnp.float32),
            pltpu.VMEM((2, 2, count, size, 8 * size), jnp.float32),
            pltpu.VMEM((2, 2, count - early, size, 8 * size), jnp.float32),
            pltpu.VMEM((2, count, 3 * size, 8 * size), jnp.bfloat16),
            pltpu.VMEM((4, count, 3 * size, 8 * size), jnp.bfloat16),
            pltpu.VMEM((2, early, size, 8 * size), jnp.float32),
            pltpu.VMEM((4, count, 3 * size, 8 * size), jnp.bfloat16),
            dma((2,)), dma, dma, dma, dma, dma((4, GROUPS)), dma, dma((GROUPS,)), dma, dma((3, steps)),
            dma, dma, dma((4, pieces)), dma, dma((steps,)), dma, dma((steps,)), dma, dma,
        ],
        compiler_params=pltpu.CompilerParams(
            collective_id=0, has_side_effects=True, vmem_limit_bytes=24000000
        ),
        name="overlap",
    )(stay(orbitals.reshape(parts, orbs, cells)), stay(potential))
    inter, applied = pl.pallas_call(
        publish,
        out_shape=(
            jax.ShapeDtypeStruct((half, 2, rows), jnp.float32),
            jax.ShapeDtypeStruct((parts, orbs, cells), jnp.bfloat16),
        ),
        in_specs=[vmem, vmem],
        out_specs=[pl.BlockSpec(memory_space=pltpu.HBM)] * 2,
        scratch_shapes=[pltpu.VMEM((half, 2, rows), jnp.float32), dma((2,))],
        compiler_params=pltpu.CompilerParams(vmem_limit_bytes=16000000),
        name="publish",
    )(inter, applied)
    return inter, applied.reshape(orbitals.shape)


def solution(mesh):
    in_specs = (P(None, ("row", "col"), "depth", None), P("depth", None))
    out_specs = (P(("row", "depth"), None, "col"), P(None, ("row", "col"), "depth", None))
    sizes = tuple(mesh.shape[axis] for axis in ("row", "col", "depth"))
    body = exchange if sizes == (4, 4, 2) else shards
    return jax.shard_map(body, mesh=mesh, in_specs=in_specs, out_specs=out_specs, check_vma=False)
```

```python
import functools

import jax
import jax.numpy as jnp
from jax import lax
from jax.experimental import pallas as pl
from jax.experimental.pallas import tpu as pltpu
from jax.sharding import PartitionSpec as P

NX = 64
MESH = pl.DeviceIdType.MESH


def with_halo(block, sides, width):
    for axis, dim in sides:
        count = lax.axis_size(axis)
        forward = [(i, i + 1) for i in range(count - 1)]
        forward.append((count - 1, 0))
        backward = [(target, source) for source, target in forward]
        low = lax.ppermute(
            lax.slice_in_dim(block, block.shape[dim] - width, None, axis=dim), axis, forward
        )
        high = lax.ppermute(lax.slice_in_dim(block, 0, width, axis=dim), axis, backward)
        block = jnp.concatenate([low, block, high], axis=dim)
    return block


def apply_operator(padded, potential):
    center = padded[:, :, 1:-1].astype(jnp.float32)
    below = padded[:, :, :-2].astype(jnp.float32)
    above = padded[:, :, 2:].astype(jnp.float32)
    flat_cells = center.shape[-1]
    xpos = jnp.arange(flat_cells) % NX
    yminus = jnp.roll(center, NX, axis=3)
    yplus = jnp.roll(center, -NX, axis=3)
    xminus = jnp.where(xpos == 0, jnp.roll(center, 1 - NX, axis=3), jnp.roll(center, 1, axis=3))
    xplus = jnp.where(
        xpos == NX - 1, jnp.roll(center, NX - 1, axis=3), jnp.roll(center, -1, axis=3)
    )
    lap = below + above + yminus + yplus + xminus + xplus - 6.0 * center
    return (-0.5 * lap + potential[None, None] * center).astype(jnp.bfloat16)


def contract(left, right):
    return lax.dot_general(
        left, right, (((1,), (1,)), ((), ())), preferred_element_type=jnp.float32
    )


def shards(orbitals, potential):
    parts, orbs, planes, cells = orbitals.shape
    flat = orbitals.reshape(parts, orbs, planes * cells)
    panel = lax.all_gather(flat, "col", axis=1, tiled=True)
    other = lax.all_gather(flat, "row", axis=1, tiled=True)
    padded = with_halo(orbitals, (("depth", 2),), 1)
    applied = apply_operator(padded, potential)
    dvol = 1.0 / (planes * lax.axis_size("depth") * cells)
    tile_cols = other.shape[1]
    real_rows = panel[0]
    imag_rows = panel[1]
    sreal = contract(real_rows, other[0]) + contract(imag_rows, other[1])
    simag = contract(real_rows, other[1]) - contract(imag_rows, other[0])
    summed = lax.psum_scatter(
        dvol * jnp.concatenate([sreal, simag], axis=1), "depth", scatter_dimension=0, tiled=True
    )
    intersection = summed.reshape(summed.shape[0], 2, tile_cols)
    intersection = lax.all_to_all(intersection, "col", split_axis=2, concat_axis=2, tiled=True)
    return (intersection, applied)


def flip(a, b):
    low = lax.rem(lax.rem(a, 2) + lax.rem(b, 2), 2)
    high = lax.rem(lax.div(a, 2) + lax.div(b, 2), 2)
    return 2 * high + low


def stencil(orb, halo, pot, out):
    parts, orbs, cells = orb.shape
    step = 16
    xpos = lax.broadcasted_iota(jnp.int32, (step, cells), 1) % NX
    first, last = xpos == 0, xpos == NX - 1

    def body(i, carry):
        part = lax.div(i, orbs // step)
        rows = pl.ds(pl.multiple_of(lax.rem(i, orbs // step) * step, step), step)
        center = orb[part, rows, :].astype(jnp.float32)
        side = halo[part, rows, :].astype(jnp.float32)
        right = pltpu.roll(center, 1, 1)
        left = pltpu.roll(center, cells - 1, 1)
        yminus = pltpu.roll(center, NX, 1)
        yplus = pltpu.roll(center, cells - NX, 1)
        xminus = jnp.where(first, pltpu.roll(right, cells - NX, 1), right)
        xplus = jnp.where(last, pltpu.roll(left, NX, 1), left)
        lap = side + side + yminus + yplus + xminus + xplus - 6.0 * center
        out[part, rows, :] = (-0.5 * lap + pot[0:1, :] * center).astype(out.dtype)
        return carry

    lax.fori_loop(0, parts * (orbs // step), body, 0)


STAGES = ((0, 2), (2, 3), (3, 4))
PIECES = ((0, 0, 4), (1, 0, 5), (2, 0, 4), (2, 4, 3))
GROUPS = 4
OUTER, INNER = 0, 1
MEMBERS = (
    ((OUTER, 0), (OUTER, 1)),
    ((OUTER, 2), (INNER, 0)),
    ((OUTER, 3), (INNER, 1)),
    ((INNER, 2), (INNER, 3)),
)
CUTS = ((0, 0, 2), (1, 0, 2), (2, 0, 2), (3, 0, 1), (3, 1, 1))
PLACE = {member: (g, u) for g, pair in enumerate(MEMBERS) for u, member in enumerate(pair)}


def blocks():
    order, spans = {}, []
    for low, high in STAGES:
        begin = len(order)
        for a in range(high):
            for b in range(high):
                if max(a, b) >= low:
                    order[a, b] = len(order)
        spans.append((begin, len(order) - begin))
    return order, spans


def kernel(dvol, orb_hbm, pot_hbm, inter, applied, orb, pot, halo, panel, acc, take, pacc, cross,
           land, relay, ptake, ins, hs, hr, ls, zs, zr, xs, xr, ds, dr, gs, gr, qr, rs, rr, ps, pr, fs, fr):
    r, c, d = lax.axis_index("row"), lax.axis_index("col"), lax.axis_index("depth")
    parts, orbs, cells = orb.shape
    quarter = cells // 4
    size = orbs // GROUPS
    wide = 8 * size
    order, spans = blocks()
    load = pltpu.make_async_copy(orb_hbm, orb, ins.at[0])
    load.start()
    load_pot = pltpu.make_async_copy(pot_hbm, pot, ins.at[1])
    load_pot.start()
    peer = (r, c, 1 - d)
    zdev = [None] + [(r, flip(c, k), d) for k in (1, 2, 3)]
    xdev = [None] + [(flip(r, k), c, d) for k in (1, 2)]

    barrier = pltpu.get_barrier_semaphore()
    friends = [peer] + zdev[1:] + xdev[1:] + [(flip(r, k), c, 1 - d) for k in (1, 2)]
    for dev in friends:
        pl.semaphore_signal(barrier, inc=1, device_id=dev, device_id_type=MESH)
    load.wait()
    pl.semaphore_wait(barrier, len(friends))

    def send(src, dst, ssem, rsem, dev):
        return pltpu.make_async_remote_copy(
            src_ref=src, dst_ref=dst, send_sem=ssem, recv_sem=rsem,
            device_id=dev, device_id_type=MESH,
        )

    def own(m, k, begin=0, count=2):
        half = quarter // 2
        lanes = pl.ds(pl.multiple_of(k * quarter + begin * half, half), count * half)
        return orb.at[:, pl.ds(m * size, size), lanes]

    def place(m, k):
        deep = lax.rem(k + 1, 4) >= 2
        return [jnp.where(deep, i, o) for i, o in zip(PLACE[INNER, m], PLACE[OUTER, m])]

    def home(m, k):
        return place(m, k)[0]

    def spot(j, m, k, begin=0, count=2):
        g, u = place(m, k)
        half = quarter // 2
        return panel.at[j, g, :, u, lax.div(k, 2), :, pl.ds(begin * half, count * half)]

    def go(cp):
        cp.start()
        return cp

    def flush(ref, sem):
        pltpu.make_async_copy(ref, ref, sem).wait()

    zsend = {}
    for n, (m, *cut) in enumerate(CUTS):
        for k in (1, 3, 2):
            zsend[k, n] = go(send(own(m, flip(c, k), *cut), spot(0, m, c, *cut), zs, zr.at[k, n], zdev[k]))
    for g in range(GROUPS):
        for j in (1, 2):
            send(own(g, c), spot(j, g, c), xs, xr.at[home(g, c)], xdev[j]).start()
    edge = send(orb, halo, hs, hr, peer)
    edge.start()
    for g in range(GROUPS):
        pltpu.make_async_copy(own(g, c), spot(0, g, c), ls).start()

    inner = lax.rem(c + 1, 4) >= 2
    lane = lax.broadcasted_iota(jnp.int32, (1, 2 * wide // 2), 1)
    sign = jnp.where(lane < wide // 2, 1.0, -1.0).astype(jnp.float32)

    def fold(x):
        rows = x.shape[0] // 2
        return x[:rows] + sign * pltpu.roll(x[rows:], wide // 2, 1)

    def span(s):
        begin, count = spans[s]
        return pl.ds(begin, count)

    def forward(k, n):
        zsend[k, n].wait_recv()
        m, *cut = CUTS[n]
        for j in (1, 2):
            part = [spot(i, m, flip(c, k), *cut) for i in (0, j)]
            send(*part, xs, xr.at[home(m, flip(c, k))], xdev[j]).start()

    def forwards(deep, shallow):
        @pl.when(inner)
        def _():
            for k, m in deep:
                forward(k, m)

        @pl.when(jnp.logical_not(inner))
        def _():
            for k, m in shallow:
                forward(k, m)

    last = len(STAGES) - 1

    def gathered(g):
        flush(panel.at[1:3, g], xr.at[g])

    def fresh(s):
        return [(a, b) for a, b in order if spans[s][0] <= order[a, b] < sum(spans[s])]

    def tile(t, s):
        top = STAGES[s][1]
        left = panel[0, 0:top].reshape(top * wide, quarter)
        right = panel[t, 0:top].reshape(top * wide, quarter)
        prod = contract(left, right)
        for a, b in fresh(s):
            x = fold(prod[a * wide:(a + 1) * wide, b * wide:(b + 1) * wide])
            x = x.reshape(2, 2, size, wide)
            for h in (0, 1):
                acc[t, h, order[a, b]] = x[:, h].reshape(2 * size, wide)
        send(acc.at[t, 1 - d, span(s)], take.at[t, span(s)], ds, dr.at[t, s], peer).start()

    def shared(s):
        top, half = STAGES[s][1], wide // 2
        for j in (1, 2):
            left = panel[j, 0:top, :, j - 1].reshape(top * half, quarter)
            right = panel[3 - j, 0:top].reshape(top * wide, quarter)
            prod = contract(left, right)
            for a, b in fresh(s):
                x = fold(prod[a * half:(a + 1) * half, b * wide:(b + 1) * wide])
                for h in (0, 1):
                    pacc[h, j - 1, order[a, b]] = x[h * size:(h + 1) * size]
            if s == last:
                for h in (0, 1):
                    dev = (flip(r, jnp.int32(j)), c, jnp.int32(h))
                    send(pacc.at[h, j - 1, span(s)], cross.at[j - 1, d], fs, fr, dev).start()
        if s < last:
            send(pacc.at[1 - d, :, span(s)], ptake.at[:, span(s)], ps, pr.at[s], peer).start()

    def settle(t, s):
        flush(take.at[t, span(s)], dr.at[t, s])
        acc[t, d, span(s)] += take[t, span(s)]

    def swap(s):
        flush(ptake.at[:, span(s)], pr.at[s])
        pacc[d, :, span(s)] += ptake[:, span(s)]
        for j in (1, 2):
            dst = acc.at[3, d, span(s), pl.ds((j - 1) * size, size)]
            send(pacc.at[d, j - 1, span(s)], dst, rs, rr.at[s], xdev[j]).start()

    def swapped(s):
        if s < last:
            flush(acc.at[3, d, span(s)], rr.at[s])
        else:
            flush(cross, fr)
            for j in (0, 1):
                acc[3, d, span(s), pl.ds(j * size, size)] = cross[j, 0] + cross[j, 1]

    def route(t):
        to = flip(r, jnp.asarray(t, jnp.int32))
        return to, lax.div(to, 2) != lax.div(c, 2)

    def chunk(n):
        s, skip, count = PIECES[n]
        return pl.ds(spans[s][0] + skip, count)

    def far(t, s, side=True):
        to, across = route(t)

        @pl.when(jnp.logical_and(jnp.logical_and(across, jnp.logical_not(inner)), side))
        def _():
            for n in range(len(PIECES)):
                if PIECES[n][0] == s:
                    send(acc.at[t, d, chunk(n)], relay.at[t, chunk(n)], gs, qr.at[t, n], zdev[1]).start()

    def near(t, s, side=True):
        to, across = route(t)

        @pl.when(jnp.logical_and(jnp.logical_and(to != c, jnp.logical_not(across)), side))
        def _():
            send(acc.at[t, d, span(s)], land.at[0, span(s)], gs, gr, zdev[1]).start()

    def pass_on(t, n, side=True):
        to, across = route(t)

        @pl.when(jnp.logical_and(jnp.logical_and(across, inner), side))
        def _():
            flush(relay.at[t, chunk(n)], qr.at[t, n])
            acc[t, d, chunk(n)] += relay[t, chunk(n)]
            send(acc.at[t, d, chunk(n)], land.at[1, chunk(n)], gs, gr, (r, to, d)).start()

    deep, edge_chip = inner, jnp.logical_not(inner)
    first = jnp.where(lax.div(r, 2) == lax.div(c, 2), 2, 1)
    second = 3 - first

    def operator():
        load_pot.wait()
        edge.wait()
        stencil(orb, halo, pot, applied)
        flush(panel.at[0, 0], ls)

    operator()
    forwards(((1, 0), (3, 0), (2, 0), (1, 1), (2, 1), (1, 2), (2, 2)), ((1, 0), (3, 0), (2, 0), (3, 1), (1, 1), (3, 2)))
    tile(0, 0)
    forwards(((1, 3), (2, 3)), ((1, 2), (1, 3), (1, 4)))
    settle(0, 0)
    far(0, 0)
    near(0, 0)
    gathered(0)
    gathered(1)
    shared(0)
    forwards(((1, 4), (2, 4)), ((3, 3), (3, 4)))
    tile(first, 0)
    forwards((), ((2, 1),))
    tile(second, 0)
    forwards(((3, 1),), ())
    swap(0)
    settle(first, 0)
    far(first, 0)
    settle(second, 0)
    far(second, 0)
    near(2, 0)
    near(1, 0)
    tile(0, 1)
    forwards(((3, 2),), ((2, 2),))
    settle(0, 1)
    far(0, 1)
    near(0, 1)
    forwards(((3, 3),), ((2, 3),))
    gathered(2)
    shared(1)
    forwards(((3, 4),), ((2, 4),))
    swapped(0)
    far(3, 0)
    near(3, 0)
    pass_on(0, 0)
    tile(first, 1)
    pass_on(2, 0)
    pass_on(1, 0)
    tile(second, 1)
    swap(1)
    settle(first, 1)
    far(first, 1)
    pass_on(3, 0)
    pass_on(0, 1)
    tile(0, 2)
    settle(second, 1)
    far(second, 1)
    near(2, 1, deep)
    near(1, 1, deep)
    gathered(3)
    shared(2)
    swapped(1)
    far(3, 1)
    near(3, 1, deep)
    tile(first, 2)
    settle(0, 2)
    far(0, 2)
    near(0, 2, deep)
    pass_on(first, 1)
    tile(second, 2)
    pass_on(second, 1)
    settle(first, 2)
    far(first, 2)
    near(2, 2, jnp.logical_and(deep, first == 2))
    near(1, 2, jnp.logical_and(deep, first == 1))
    settle(second, 2)
    far(second, 2)
    near(2, 2, jnp.logical_and(deep, first == 1))
    near(1, 2, jnp.logical_and(deep, first == 2))
    pass_on(3, 1)
    near(3, 1, edge_chip)
    near(2, 1, edge_chip)
    near(2, 2, edge_chip)
    pass_on(0, 2)
    pass_on(0, 3)
    swapped(2)
    far(3, 2)
    near(3, 2)
    near(1, 1, edge_chip)
    near(0, 2, edge_chip)
    near(1, 2, edge_chip)
    pass_on(first, 2)
    pass_on(first, 3)
    pass_on(3, 2)
    pass_on(3, 3)
    pass_on(second, 2)
    pass_on(second, 3)

    flush(panel.at[0, 0:3], zs)
    flush(panel.at[0:2], xs)
    flush(take, ds)
    flush(acc.at[3, 0, 0:spans[last][0]], rs)
    flush(ptake, ps)
    flush(cross, fs)
    mine = flip(r, c)
    flush(land, gr)
    acc[mine, d] = (acc[mine, d] + land[0] + land[1]) * dvol
    half, quad = wide // 2, wide // 8
    pick = lax.div(lane, quad)
    for a in range(GROUPS):
        for u, (kind, m) in enumerate(MEMBERS[a]):
            total = []
            for b in range(GROUPS):
                i, rows = order[a, b], pl.ds(u * size, size)
                total.append(acc[mine, d, i, rows])
            first = (d if kind == OUTER else 1 - d) * half + m * size
            for part in range(parts):
                for v in (0, 1):
                    out = None
                    for b in range(GROUPS):
                        for w, (col, n) in enumerate(MEMBERS[b]):
                            at = part * half + w * 2 * quad + v * quad
                            to = (col ^ v) * half + n * quad
                            moved = pltpu.roll(total[b], (to - at) % wide, 1)
                            out = moved if out is None else jnp.where(pick == to // quad, moved, out)
                    rows = pl.ds(pl.multiple_of(first, size), size)
                    inter[rows, part, pl.ds(v * wide, wide)] = out

    flush(relay.at[0:3], gs)


def publish(inter, applied, inter_out, applied_out, sems):
    copies = [
        pltpu.make_async_copy(applied, applied_out, sems.at[0]),
        pltpu.make_async_copy(inter, inter_out, sems.at[1]),
    ]
    for cp in copies:
        cp.start()
    for cp in copies:
        cp.wait()


def stay(array):
    return pltpu.with_memory_space_constraint(array, pltpu.HBM)


def exchange(orbitals, potential):
    parts, orbs, planes, cells = orbitals.shape
    rows = orbs * lax.axis_size("col")
    half = rows // 2
    size = orbs // GROUPS
    count = GROUPS * GROUPS
    steps, pieces = len(STAGES), len(PIECES)
    dvol = 1.0 / (planes * lax.axis_size("depth") * cells)
    vmem = pl.BlockSpec(memory_space=pltpu.VMEM)
    dma = pltpu.SemaphoreType.DMA
    block = (count, 2 * size, 8 * size)
    early = blocks()[1][-1][0]
    inter, applied = pl.pallas_call(
        functools.partial(kernel, dvol),
        out_shape=(
            jax.ShapeDtypeStruct((half, 2, rows), jnp.float32),
            jax.ShapeDtypeStruct((parts, orbs, cells), jnp.bfloat16),
        ),
        in_specs=[pl.BlockSpec(memory_space=pltpu.HBM)] * 2,
        out_specs=(vmem, vmem),
        scratch_shapes=[
            pltpu.VMEM((parts, orbs, cells), jnp.bfloat16),
            pltpu.VMEM(potential.shape, jnp.float32),
            pltpu.VMEM((parts, orbs, cells), jnp.bfloat16),
            pltpu.VMEM((3, GROUPS, parts, 2, 2, size, cells // 4), jnp.bfloat16),
            pltpu.VMEM((4, 2) + block, jnp.float32),
            pltpu.VMEM((3,) + block, jnp.float32),
            pltpu.VMEM((2, 2, count, size, 8 * size), jnp.float32),
            pltpu.VMEM((2, 2, count - early, size, 8 * size), jnp.float32),
            pltpu.VMEM((2,) + block, jnp.float32),
            pltpu.VMEM((4,) + block, jnp.float32),
            pltpu.VMEM((2, early, size, 8 * size), jnp.float32),
            dma((2,)), dma, dma, dma, dma, dma((4, len(CUTS))), dma, dma((GROUPS,)), dma, dma((3, steps)),
            dma, dma, dma((4, pieces)), dma, dma((steps,)), dma, dma((steps,)), dma, dma,
        ],
        compiler_params=pltpu.CompilerParams(
            collective_id=0, has_side_effects=True, vmem_limit_bytes=24000000
        ),
        name="overlap",
    )(stay(orbitals.reshape(parts, orbs, cells)), stay(potential))
    inter, applied = pl.pallas_call(
        publish,
        out_shape=(
            jax.ShapeDtypeStruct((half, 2, rows), jnp.float32),
            jax.ShapeDtypeStruct((parts, orbs, cells), jnp.bfloat16),
        ),
        in_specs=[vmem, vmem],
        out_specs=[pl.BlockSpec(memory_space=pltpu.HBM)] * 2,
        scratch_shapes=[dma((2,))],
        compiler_params=pltpu.CompilerParams(vmem_limit_bytes=16000000),
        name="publish",
    )(inter, applied)
    return inter, applied.reshape(orbitals.shape)


def solution(mesh):
    in_specs = (P(None, ("row", "col"), "depth", None), P("depth", None))
    out_specs = (P(("row", "depth"), None, "col"), P(None, ("row", "col"), "depth", None))
    sizes = tuple(mesh.shape[axis] for axis in ("row", "col", "depth"))
    body = exchange if sizes == (4, 4, 2) else shards
    return jax.shard_map(body, mesh=mesh, in_specs=in_specs, out_specs=out_specs, check_vma=False)
```

```python
import functools

import jax
import jax.numpy as jnp
from jax import lax
from jax.experimental import pallas as pl
from jax.experimental.pallas import tpu as pltpu
from jax.sharding import PartitionSpec as P

NX = 64
MESH = pl.DeviceIdType.MESH


def with_halo(block, sides, width):
    for axis, dim in sides:
        count = lax.axis_size(axis)
        forward = [(i, i + 1) for i in range(count - 1)]
        forward.append((count - 1, 0))
        backward = [(target, source) for source, target in forward]
        low = lax.ppermute(
            lax.slice_in_dim(block, block.shape[dim] - width, None, axis=dim), axis, forward
        )
        high = lax.ppermute(lax.slice_in_dim(block, 0, width, axis=dim), axis, backward)
        block = jnp.concatenate([low, block, high], axis=dim)
    return block


def apply_operator(padded, potential):
    center = padded[:, :, 1:-1].astype(jnp.float32)
    below = padded[:, :, :-2].astype(jnp.float32)
    above = padded[:, :, 2:].astype(jnp.float32)
    flat_cells = center.shape[-1]
    xpos = jnp.arange(flat_cells) % NX
    yminus = jnp.roll(center, NX, axis=3)
    yplus = jnp.roll(center, -NX, axis=3)
    xminus = jnp.where(xpos == 0, jnp.roll(center, 1 - NX, axis=3), jnp.roll(center, 1, axis=3))
    xplus = jnp.where(
        xpos == NX - 1, jnp.roll(center, NX - 1, axis=3), jnp.roll(center, -1, axis=3)
    )
    lap = below + above + yminus + yplus + xminus + xplus - 6.0 * center
    return (-0.5 * lap + potential[None, None] * center).astype(jnp.bfloat16)


def contract(left, right):
    return lax.dot_general(
        left, right, (((1,), (1,)), ((), ())), preferred_element_type=jnp.float32
    )


def shards(orbitals, potential):
    parts, orbs, planes, cells = orbitals.shape
    flat = orbitals.reshape(parts, orbs, planes * cells)
    panel = lax.all_gather(flat, "col", axis=1, tiled=True)
    other = lax.all_gather(flat, "row", axis=1, tiled=True)
    padded = with_halo(orbitals, (("depth", 2),), 1)
    applied = apply_operator(padded, potential)
    dvol = 1.0 / (planes * lax.axis_size("depth") * cells)
    tile_cols = other.shape[1]
    real_rows = panel[0]
    imag_rows = panel[1]
    sreal = contract(real_rows, other[0]) + contract(imag_rows, other[1])
    simag = contract(real_rows, other[1]) - contract(imag_rows, other[0])
    summed = lax.psum_scatter(
        dvol * jnp.concatenate([sreal, simag], axis=1), "depth", scatter_dimension=0, tiled=True
    )
    intersection = summed.reshape(summed.shape[0], 2, tile_cols)
    intersection = lax.all_to_all(intersection, "col", split_axis=2, concat_axis=2, tiled=True)
    return (intersection, applied)


def flip(a, b):
    low = lax.rem(lax.rem(a, 2) + lax.rem(b, 2), 2)
    high = lax.rem(lax.div(a, 2) + lax.div(b, 2), 2)
    return 2 * high + low


def stencil(orb, halo, pot, out):
    parts, orbs, cells = orb.shape
    step = 16
    xpos = lax.broadcasted_iota(jnp.int32, (step, cells), 1) % NX
    first, last = xpos == 0, xpos == NX - 1

    def body(i, carry):
        part = lax.div(i, orbs // step)
        rows = pl.ds(pl.multiple_of(lax.rem(i, orbs // step) * step, step), step)
        center = orb[part, rows, :].astype(jnp.float32)
        side = halo[part, rows, :].astype(jnp.float32)
        right = pltpu.roll(center, 1, 1)
        left = pltpu.roll(center, cells - 1, 1)
        yminus = pltpu.roll(center, NX, 1)
        yplus = pltpu.roll(center, cells - NX, 1)
        xminus = jnp.where(first, pltpu.roll(right, cells - NX, 1), right)
        xplus = jnp.where(last, pltpu.roll(left, NX, 1), left)
        lap = side + side + yminus + yplus + xminus + xplus - 6.0 * center
        out[part, rows, :] = (-0.5 * lap + pot[0:1, :] * center).astype(out.dtype)
        return carry

    lax.fori_loop(0, parts * (orbs // step), body, 0)


STAGES = ((0, 2), (2, 3), (3, 4))
PIECES = ((0, 0, 4), (1, 0, 5), (2, 0, 4), (2, 4, 3))
GROUPS = 4
OUTER, INNER = 0, 1
MEMBERS = (
    ((OUTER, 0), (OUTER, 1)),
    ((OUTER, 2), (INNER, 0)),
    ((OUTER, 3), (INNER, 1)),
    ((INNER, 2), (INNER, 3)),
)
CUTS = ((0, 0, 2), (1, 0, 2), (2, 0, 2), (3, 0, 1), (3, 1, 1))
PLACE = {member: (g, u) for g, pair in enumerate(MEMBERS) for u, member in enumerate(pair)}


def blocks():
    order, spans = {}, []
    for low, high in STAGES:
        begin = len(order)
        for a in range(high):
            for b in range(high):
                if max(a, b) >= low:
                    order[a, b] = len(order)
        spans.append((begin, len(order) - begin))
    return order, spans


def kernel(dvol, orb_hbm, pot_hbm, inter, applied, orb, pot, halo, panel, acc, take, pacc, cross,
           land, relay, ptake, wire, ins, hs, hr, ls, zs, zr, xs, xr, ds, dr, gs, gr, qr, rs, rr, ps, pr, fs, fr):
    r, c, d = lax.axis_index("row"), lax.axis_index("col"), lax.axis_index("depth")
    parts, orbs, cells = orb.shape
    quarter = cells // 4
    size = orbs // GROUPS
    wide = 8 * size
    order, spans = blocks()
    load = pltpu.make_async_copy(orb_hbm, orb, ins.at[0])
    load.start()
    load_pot = pltpu.make_async_copy(pot_hbm, pot, ins.at[1])
    load_pot.start()
    peer = (r, c, 1 - d)
    zdev = [None] + [(r, flip(c, k), d) for k in (1, 2, 3)]
    xdev = [None] + [(flip(r, k), c, d) for k in (1, 2)]

    barrier = pltpu.get_barrier_semaphore()
    friends = [peer] + zdev[1:] + xdev[1:] + [(flip(r, k), c, 1 - d) for k in (1, 2)]
    for dev in friends:
        pl.semaphore_signal(barrier, inc=1, device_id=dev, device_id_type=MESH)
    load.wait()
    pl.semaphore_wait(barrier, len(friends))

    def send(src, dst, ssem, rsem, dev):
        return pltpu.make_async_remote_copy(
            src_ref=src, dst_ref=dst, send_sem=ssem, recv_sem=rsem,
            device_id=dev, device_id_type=MESH,
        )

    def own(m, k, begin=0, count=2):
        half = quarter // 2
        lanes = pl.ds(pl.multiple_of(k * quarter + begin * half, half), count * half)
        return orb.at[:, pl.ds(m * size, size), lanes]

    def place(m, k):
        deep = lax.rem(k + 1, 4) >= 2
        return [jnp.where(deep, i, o) for i, o in zip(PLACE[INNER, m], PLACE[OUTER, m])]

    def home(m, k):
        return place(m, k)[0]

    def spot(j, m, k, begin=0, count=2):
        g, u = place(m, k)
        half = quarter // 2
        return panel.at[j, g, :, u, lax.div(k, 2), :, pl.ds(begin * half, count * half)]

    def go(cp):
        cp.start()
        return cp

    def flush(ref, sem):
        pltpu.make_async_copy(ref, ref, sem).wait()

    zsend = {}
    for n, (m, *cut) in enumerate(CUTS):
        for k in (1, 3, 2):
            zsend[k, n] = go(send(own(m, flip(c, k), *cut), spot(0, m, c, *cut), zs, zr.at[k, n], zdev[k]))
    for g in range(GROUPS):
        for j in (1, 2):
            send(own(g, c), spot(j, g, c), xs, xr.at[home(g, c)], xdev[j]).start()
    edge = send(orb, halo, hs, hr, peer)
    edge.start()
    for g in range(GROUPS):
        pltpu.make_async_copy(own(g, c), spot(0, g, c), ls).start()

    inner = lax.rem(c + 1, 4) >= 2
    lane = lax.broadcasted_iota(jnp.int32, (1, 2 * wide // 2), 1)
    sign = jnp.where(lane < wide // 2, 1.0, -1.0).astype(jnp.float32)

    def fold(x):
        rows = x.shape[0] // 2
        return x[:rows] + sign * pltpu.roll(x[rows:], wide // 2, 1)

    def span(s):
        begin, count = spans[s]
        return pl.ds(begin, count)

    def forward(k, n):
        zsend[k, n].wait_recv()
        m, *cut = CUTS[n]
        for j in (1, 2):
            part = [spot(i, m, flip(c, k), *cut) for i in (0, j)]
            send(*part, xs, xr.at[home(m, flip(c, k))], xdev[j]).start()

    def forwards(deep, shallow):
        @pl.when(inner)
        def _():
            for k, m in deep:
                forward(k, m)

        @pl.when(jnp.logical_not(inner))
        def _():
            for k, m in shallow:
                forward(k, m)

    last = len(STAGES) - 1

    def gathered(g):
        flush(panel.at[1:3, g], xr.at[g])

    def fresh(s):
        return [(a, b) for a, b in order if spans[s][0] <= order[a, b] < sum(spans[s])]

    def tile(t, s):
        top = STAGES[s][1]
        left = panel[0, 0:top].reshape(top * wide, quarter)
        right = panel[t, 0:top].reshape(top * wide, quarter)
        prod = contract(left, right)
        for a, b in fresh(s):
            x = fold(prod[a * wide:(a + 1) * wide, b * wide:(b + 1) * wide])
            x = x.reshape(2, 2, size, wide)
            for h in (0, 1):
                acc[t, h, order[a, b]] = x[:, h].reshape(2 * size, wide)
        send(acc.at[t, 1 - d, span(s)], take.at[t, span(s)], ds, dr.at[t, s], peer).start()

    def shared(s):
        top, half = STAGES[s][1], wide // 2
        for j in (1, 2):
            left = panel[j, 0:top, :, j - 1].reshape(top * half, quarter)
            right = panel[3 - j, 0:top].reshape(top * wide, quarter)
            prod = contract(left, right)
            for a, b in fresh(s):
                x = fold(prod[a * half:(a + 1) * half, b * wide:(b + 1) * wide])
                for h in (0, 1):
                    pacc[h, j - 1, order[a, b]] = x[h * size:(h + 1) * size]
            if s == last:
                for h in (0, 1):
                    dev = (flip(r, jnp.int32(j)), c, jnp.int32(h))
                    send(pacc.at[h, j - 1, span(s)], cross.at[j - 1, d], fs, fr, dev).start()
        if s < last:
            send(pacc.at[1 - d, :, span(s)], ptake.at[:, span(s)], ps, pr.at[s], peer).start()

    def settle(t, s):
        flush(take.at[t, span(s)], dr.at[t, s])
        acc[t, d, span(s)] += take[t, span(s)]

    def swap(s):
        flush(ptake.at[:, span(s)], pr.at[s])
        pacc[d, :, span(s)] += ptake[:, span(s)]
        for j in (1, 2):
            dst = acc.at[3, d, span(s), pl.ds((j - 1) * size, size)]
            send(pacc.at[d, j - 1, span(s)], dst, rs, rr.at[s], xdev[j]).start()

    def swapped(s):
        if s < last:
            flush(acc.at[3, d, span(s)], rr.at[s])
        else:
            flush(cross, fr)
            for j in (0, 1):
                acc[3, d, span(s), pl.ds(j * size, size)] = cross[j, 0] + cross[j, 1]

    def encode(t, blocks):
        x = acc[t, d, blocks]
        high = x.astype(jnp.bfloat16)
        base = high.astype(jnp.float32)
        steps = jnp.round((x - base) / jnp.maximum(jnp.abs(base), 1e-37) * 2048.0)
        steps = jnp.clip(steps, -7.0, 7.0)
        wire[t, blocks, :2 * size] = high
        wire[t, blocks, 2 * size:] = (steps[:, :size] * 16.0 + steps[:, size:]).astype(jnp.bfloat16)

    def decode(words):
        base = words[:, :2 * size].astype(jnp.float32)
        code = words[:, 2 * size:].astype(jnp.float32)
        upper = jnp.round(code / 16.0)
        steps = jnp.concatenate([upper, code - 16.0 * upper], axis=1)
        return base + steps * jnp.abs(base) / 2048.0

    def route(t):
        to = flip(r, jnp.asarray(t, jnp.int32))
        return to, lax.div(to, 2) != lax.div(c, 2)

    def chunk(n):
        s, skip, count = PIECES[n]
        return pl.ds(spans[s][0] + skip, count)

    def far(t, s, side=True):
        to, across = route(t)

        @pl.when(jnp.logical_and(jnp.logical_and(across, jnp.logical_not(inner)), side))
        def _():
            for n in range(len(PIECES)):
                if PIECES[n][0] == s:
                    encode(t, chunk(n))
                    send(wire.at[t, chunk(n)], relay.at[t, chunk(n)], gs, qr.at[t, n], zdev[1]).start()

    def near(t, s, side=True):
        to, across = route(t)

        @pl.when(jnp.logical_and(jnp.logical_and(to != c, jnp.logical_not(across)), side))
        def _():
            encode(t, span(s))
            send(wire.at[t, span(s)], land.at[0, span(s)], gs, gr, zdev[1]).start()

    def pass_on(t, n, side=True):
        to, across = route(t)

        @pl.when(jnp.logical_and(jnp.logical_and(across, inner), side))
        def _():
            flush(relay.at[t, chunk(n)], qr.at[t, n])
            acc[t, d, chunk(n)] += decode(relay[t, chunk(n)])
            encode(t, chunk(n))
            send(wire.at[t, chunk(n)], land.at[1, chunk(n)], gs, gr, (r, to, d)).start()

    deep, edge_chip = inner, jnp.logical_not(inner)
    first = jnp.where(lax.div(r, 2) == lax.div(c, 2), 2, 1)
    second = 3 - first

    def operator():
        load_pot.wait()
        edge.wait()
        stencil(orb, halo, pot, applied)
        flush(panel.at[0, 0], ls)

    operator()
    forwards(((1, 0), (3, 0), (2, 0), (1, 1), (2, 1), (1, 2), (2, 2)), ((1, 0), (3, 0), (2, 0), (3, 1), (1, 1), (3, 2)))
    tile(0, 0)
    forwards(((1, 3), (2, 3)), ((1, 2), (1, 3), (1, 4)))
    settle(0, 0)
    far(0, 0)
    near(0, 0)
    gathered(0)
    gathered(1)
    shared(0)
    forwards(((1, 4), (2, 4)), ((3, 3), (3, 4)))
    tile(first, 0)
    forwards((), ((2, 1),))
    tile(second, 0)
    forwards(((3, 1),), ())
    swap(0)
    settle(first, 0)
    far(first, 0)
    settle(second, 0)
    far(second, 0)
    near(2, 0)
    near(1, 0)
    tile(0, 1)
    forwards(((3, 2),), ((2, 2),))
    settle(0, 1)
    far(0, 1)
    near(0, 1)
    forwards(((3, 3),), ((2, 3),))
    pass_on(0, 0)
    gathered(2)
    pass_on(first, 0)
    shared(1)
    forwards(((3, 4),), ((2, 4),))
    swapped(0)
    far(3, 0)
    near(3, 0)
    tile(first, 1)
    pass_on(second, 0)
    tile(second, 1)
    swap(1)
    settle(first, 1)
    far(first, 1)
    pass_on(3, 0)
    pass_on(0, 1)
    tile(0, 2)
    settle(second, 1)
    far(second, 1)
    near(2, 1, deep)
    near(1, 1, deep)
    gathered(3)
    shared(2)
    settle(0, 2)
    far(0, 2)
    near(0, 2, deep)
    swapped(1)
    far(3, 1)
    near(3, 1, deep)
    tile(first, 2)
    pass_on(first, 1)
    tile(second, 2)
    pass_on(second, 1)
    settle(first, 2)
    far(first, 2)
    near(2, 2, jnp.logical_and(deep, first == 2))
    near(1, 2, jnp.logical_and(deep, first == 1))
    settle(second, 2)
    far(second, 2)
    near(2, 2, jnp.logical_and(deep, first == 1))
    near(1, 2, jnp.logical_and(deep, first == 2))
    pass_on(3, 1)
    near(3, 1, edge_chip)
    near(2, 1, edge_chip)
    near(2, 2, edge_chip)
    pass_on(0, 2)
    pass_on(0, 3)
    swapped(2)
    far(3, 2)
    near(3, 2)
    near(1, 1, edge_chip)
    near(0, 2, edge_chip)
    near(1, 2, edge_chip)
    pass_on(first, 2)
    pass_on(first, 3)
    pass_on(3, 2)
    pass_on(3, 3)
    pass_on(second, 2)
    pass_on(second, 3)

    flush(panel.at[0, 0:3], zs)
    flush(panel.at[0:2], xs)
    flush(take, ds)
    flush(acc.at[3, 0, 0:spans[last][0]], rs)
    flush(ptake, ps)
    flush(cross, fs)
    mine = flip(r, c)
    flush(land, gr)
    acc[mine, d] = (acc[mine, d] + decode(land[0]) + decode(land[1])) * dvol
    half, quad = wide // 2, wide // 8
    pick = lax.div(lane, quad)
    for a in range(GROUPS):
        for u, (kind, m) in enumerate(MEMBERS[a]):
            total = []
            for b in range(GROUPS):
                i, rows = order[a, b], pl.ds(u * size, size)
                total.append(acc[mine, d, i, rows])
            first = (d if kind == OUTER else 1 - d) * half + m * size
            for part in range(parts):
                for v in (0, 1):
                    out = None
                    for b in range(GROUPS):
                        for w, (col, n) in enumerate(MEMBERS[b]):
                            at = part * half + w * 2 * quad + v * quad
                            to = (col ^ v) * half + n * quad
                            moved = pltpu.roll(total[b], (to - at) % wide, 1)
                            out = moved if out is None else jnp.where(pick == to // quad, moved, out)
                    rows = pl.ds(pl.multiple_of(first, size), size)
                    inter[rows, part, pl.ds(v * wide, wide)] = out

    flush(relay.at[0:3], gs)


def publish(inter, applied, inter_out, applied_out, sems):
    copies = [
        pltpu.make_async_copy(applied, applied_out, sems.at[0]),
        pltpu.make_async_copy(inter, inter_out, sems.at[1]),
    ]
    for cp in copies:
        cp.start()
    for cp in copies:
        cp.wait()


def stay(array):
    return pltpu.with_memory_space_constraint(array, pltpu.HBM)


def exchange(orbitals, potential):
    parts, orbs, planes, cells = orbitals.shape
    rows = orbs * lax.axis_size("col")
    half = rows // 2
    size = orbs // GROUPS
    count = GROUPS * GROUPS
    steps, pieces = len(STAGES), len(PIECES)
    dvol = 1.0 / (planes * lax.axis_size("depth") * cells)
    vmem = pl.BlockSpec(memory_space=pltpu.VMEM)
    dma = pltpu.SemaphoreType.DMA
    block = (count, 2 * size, 8 * size)
    words = (count, 3 * size, 8 * size)
    early = blocks()[1][-1][0]
    inter, applied = pl.pallas_call(
        functools.partial(kernel, dvol),
        out_shape=(
            jax.ShapeDtypeStruct((half, 2, rows), jnp.float32),
            jax.ShapeDtypeStruct((parts, orbs, cells), jnp.bfloat16),
        ),
        in_specs=[pl.BlockSpec(memory_space=pltpu.HBM)] * 2,
        out_specs=(vmem, vmem),
        scratch_shapes=[
            pltpu.VMEM((parts, orbs, cells), jnp.bfloat16),
            pltpu.VMEM(potential.shape, jnp.float32),
            pltpu.VMEM((parts, orbs, cells), jnp.bfloat16),
            pltpu.VMEM((3, GROUPS, parts, 2, 2, size, cells // 4), jnp.bfloat16),
            pltpu.VMEM((4, 2) + block, jnp.float32),
            pltpu.VMEM((3,) + block, jnp.float32),
            pltpu.VMEM((2, 2, count, size, 8 * size), jnp.float32),
            pltpu.VMEM((2, 2, count - early, size, 8 * size), jnp.float32),
            pltpu.VMEM((2,) + words, jnp.bfloat16),
            pltpu.VMEM((4,) + words, jnp.bfloat16),
            pltpu.VMEM((2, early, size, 8 * size), jnp.float32),
            pltpu.VMEM((4,) + words, jnp.bfloat16),
            dma((2,)), dma, dma, dma, dma, dma((4, len(CUTS))), dma, dma((GROUPS,)), dma, dma((3, steps)),
            dma, dma, dma((4, pieces)), dma, dma((steps,)), dma, dma((steps,)), dma, dma,
        ],
        compiler_params=pltpu.CompilerParams(
            collective_id=0, has_side_effects=True, vmem_limit_bytes=24000000
        ),
        name="overlap",
    )(stay(orbitals.reshape(parts, orbs, cells)), stay(potential))
    inter, applied = pl.pallas_call(
        publish,
        out_shape=(
            jax.ShapeDtypeStruct((half, 2, rows), jnp.float32),
            jax.ShapeDtypeStruct((parts, orbs, cells), jnp.bfloat16),
        ),
        in_specs=[vmem, vmem],
        out_specs=[pl.BlockSpec(memory_space=pltpu.HBM)] * 2,
        scratch_shapes=[dma((2,))],
        compiler_params=pltpu.CompilerParams(vmem_limit_bytes=16000000),
        name="publish",
    )(inter, applied)
    return inter, applied.reshape(orbitals.shape)


def solution(mesh):
    in_specs = (P(None, ("row", "col"), "depth", None), P("depth", None))
    out_specs = (P(("row", "depth"), None, "col"), P(None, ("row", "col"), "depth", None))
    sizes = tuple(mesh.shape[axis] for axis in ("row", "col", "depth"))
    body = exchange if sizes == (4, 4, 2) else shards
    return jax.shard_map(body, mesh=mesh, in_specs=in_specs, out_specs=out_specs, check_vma=False)
```

```python
import functools

import jax
import jax.numpy as jnp
from jax import lax
from jax.experimental import pallas as pl
from jax.experimental.pallas import tpu as pltpu
from jax.sharding import PartitionSpec as P

NX = 64
MESH = pl.DeviceIdType.MESH


def with_halo(block, sides, width):
    for axis, dim in sides:
        count = lax.axis_size(axis)
        forward = [(i, i + 1) for i in range(count - 1)]
        forward.append((count - 1, 0))
        backward = [(target, source) for source, target in forward]
        low = lax.ppermute(
            lax.slice_in_dim(block, block.shape[dim] - width, None, axis=dim), axis, forward
        )
        high = lax.ppermute(lax.slice_in_dim(block, 0, width, axis=dim), axis, backward)
        block = jnp.concatenate([low, block, high], axis=dim)
    return block


def apply_operator(padded, potential):
    center = padded[:, :, 1:-1].astype(jnp.float32)
    below = padded[:, :, :-2].astype(jnp.float32)
    above = padded[:, :, 2:].astype(jnp.float32)
    flat_cells = center.shape[-1]
    xpos = jnp.arange(flat_cells) % NX
    yminus = jnp.roll(center, NX, axis=3)
    yplus = jnp.roll(center, -NX, axis=3)
    xminus = jnp.where(xpos == 0, jnp.roll(center, 1 - NX, axis=3), jnp.roll(center, 1, axis=3))
    xplus = jnp.where(
        xpos == NX - 1, jnp.roll(center, NX - 1, axis=3), jnp.roll(center, -1, axis=3)
    )
    lap = below + above + yminus + yplus + xminus + xplus - 6.0 * center
    return (-0.5 * lap + potential[None, None] * center).astype(jnp.bfloat16)


def contract(left, right):
    return lax.dot_general(
        left, right, (((1,), (1,)), ((), ())), preferred_element_type=jnp.float32
    )


def shards(orbitals, potential):
    parts, orbs, planes, cells = orbitals.shape
    flat = orbitals.reshape(parts, orbs, planes * cells)
    panel = lax.all_gather(flat, "col", axis=1, tiled=True)
    other = lax.all_gather(flat, "row", axis=1, tiled=True)
    padded = with_halo(orbitals, (("depth", 2),), 1)
    applied = apply_operator(padded, potential)
    dvol = 1.0 / (planes * lax.axis_size("depth") * cells)
    tile_cols = other.shape[1]
    real_rows = panel[0]
    imag_rows = panel[1]
    sreal = contract(real_rows, other[0]) + contract(imag_rows, other[1])
    simag = contract(real_rows, other[1]) - contract(imag_rows, other[0])
    summed = lax.psum_scatter(
        dvol * jnp.concatenate([sreal, simag], axis=1), "depth", scatter_dimension=0, tiled=True
    )
    intersection = summed.reshape(summed.shape[0], 2, tile_cols)
    intersection = lax.all_to_all(intersection, "col", split_axis=2, concat_axis=2, tiled=True)
    return (intersection, applied)


def flip(a, b):
    low = lax.rem(lax.rem(a, 2) + lax.rem(b, 2), 2)
    high = lax.rem(lax.div(a, 2) + lax.div(b, 2), 2)
    return 2 * high + low


def stencil(orb, halo, pot, out):
    parts, orbs, cells = orb.shape
    step = 16
    xpos = lax.broadcasted_iota(jnp.int32, (step, cells), 1) % NX
    first, last = xpos == 0, xpos == NX - 1

    def body(i, carry):
        part = lax.div(i, orbs // step)
        rows = pl.ds(pl.multiple_of(lax.rem(i, orbs // step) * step, step), step)
        center = orb[part, rows, :].astype(jnp.float32)
        side = halo[part, rows, :].astype(jnp.float32)
        right = pltpu.roll(center, 1, 1)
        left = pltpu.roll(center, cells - 1, 1)
        yminus = pltpu.roll(center, NX, 1)
        yplus = pltpu.roll(center, cells - NX, 1)
        xminus = jnp.where(first, pltpu.roll(right, cells - NX, 1), right)
        xplus = jnp.where(last, pltpu.roll(left, NX, 1), left)
        lap = side + side + yminus + yplus + xminus + xplus - 6.0 * center
        out[part, rows, :] = (-0.5 * lap + pot[0:1, :] * center).astype(out.dtype)
        return carry

    lax.fori_loop(0, parts * (orbs // step), body, 0)


STAGES = ((0, 2), (2, 3), (3, 4))
PIECES = ((0, 0, 4), (1, 0, 5), (2, 0, 4), (2, 4, 3))
GROUPS = 4
OUTER, INNER = 0, 1
MEMBERS = (
    ((OUTER, 0), (OUTER, 1)),
    ((OUTER, 2), (INNER, 0)),
    ((OUTER, 3), (INNER, 1)),
    ((INNER, 2), (INNER, 3)),
)
CUTS = ((0, 0, 2), (1, 0, 2), (2, 0, 2), (3, 0, 1), (3, 1, 1))
PLACE = {member: (g, u) for g, pair in enumerate(MEMBERS) for u, member in enumerate(pair)}


def blocks():
    order, spans = {}, []
    for low, high in STAGES:
        begin = len(order)
        for a in range(high):
            for b in range(high):
                if max(a, b) >= low:
                    order[a, b] = len(order)
        spans.append((begin, len(order) - begin))
    return order, spans


def kernel(dvol, orb_hbm, pot_hbm, inter, applied, orb, pot, halo, panel, acc, take, pacc, cross,
           land, relay, ptake, ins, hs, hr, ls, zs, zr, xs, xr, ds, dr, gs, gr, qr, rs, rr, ps, pr, fs, fr):
    r, c, d = lax.axis_index("row"), lax.axis_index("col"), lax.axis_index("depth")
    parts, orbs, cells = orb.shape
    quarter = cells // 4
    size = orbs // GROUPS
    wide = 8 * size
    order, spans = blocks()
    load = pltpu.make_async_copy(orb_hbm, orb, ins.at[0])
    load.start()
    load_pot = pltpu.make_async_copy(pot_hbm, pot, ins.at[1])
    load_pot.start()
    peer = (r, c, 1 - d)
    zdev = [None] + [(r, flip(c, k), d) for k in (1, 2, 3)]
    xdev = [None] + [(flip(r, k), c, d) for k in (1, 2)]

    barrier = pltpu.get_barrier_semaphore()
    friends = [peer] + zdev[1:] + xdev[1:] + [(flip(r, k), c, 1 - d) for k in (1, 2)]
    for dev in friends:
        pl.semaphore_signal(barrier, inc=1, device_id=dev, device_id_type=MESH)
    load.wait()
    pl.semaphore_wait(barrier, len(friends))

    def send(src, dst, ssem, rsem, dev):
        return pltpu.make_async_remote_copy(
            src_ref=src, dst_ref=dst, send_sem=ssem, recv_sem=rsem,
            device_id=dev, device_id_type=MESH,
        )

    def own(m, k, begin=0, count=2):
        half = quarter // 2
        lanes = pl.ds(pl.multiple_of(k * quarter + begin * half, half), count * half)
        return orb.at[:, pl.ds(m * size, size), lanes]

    def place(m, k):
        deep = lax.rem(k + 1, 4) >= 2
        return [jnp.where(deep, i, o) for i, o in zip(PLACE[INNER, m], PLACE[OUTER, m])]

    def home(m, k):
        return place(m, k)[0]

    def spot(j, m, k, begin=0, count=2):
        g, u = place(m, k)
        half = quarter // 2
        return panel.at[j, g, :, u, lax.div(k, 2), :, pl.ds(begin * half, count * half)]

    def go(cp):
        cp.start()
        return cp

    def flush(ref, sem):
        pltpu.make_async_copy(ref, ref, sem).wait()

    zsend = {}
    for n, (m, *cut) in enumerate(CUTS):
        for k in (1, 3, 2):
            zsend[k, n] = go(send(own(m, flip(c, k), *cut), spot(0, m, c, *cut), zs, zr.at[k, n], zdev[k]))
    for g in range(GROUPS):
        for j in (1, 2):
            send(own(g, c), spot(j, g, c), xs, xr.at[home(g, c)], xdev[j]).start()
    edge = send(orb, halo, hs, hr, peer)
    edge.start()
    for g in range(GROUPS):
        pltpu.make_async_copy(own(g, c), spot(0, g, c), ls).start()

    inner = lax.rem(c + 1, 4) >= 2
    lane = lax.broadcasted_iota(jnp.int32, (1, 2 * wide // 2), 1)
    sign = jnp.where(lane < wide // 2, 1.0, -1.0).astype(jnp.float32)

    def fold(x):
        rows = x.shape[0] // 2
        return x[:rows] + sign * pltpu.roll(x[rows:], wide // 2, 1)

    def span(s):
        begin, count = spans[s]
        return pl.ds(begin, count)

    def forward(k, n):
        zsend[k, n].wait_recv()
        m, *cut = CUTS[n]
        for j in (1, 2):
            part = [spot(i, m, flip(c, k), *cut) for i in (0, j)]
            send(*part, xs, xr.at[home(m, flip(c, k))], xdev[j]).start()

    def forwards(deep, shallow):
        @pl.when(inner)
        def _():
            for k, m in deep:
                forward(k, m)

        @pl.when(jnp.logical_not(inner))
        def _():
            for k, m in shallow:
                forward(k, m)

    last = len(STAGES) - 1

    def gathered(g):
        flush(panel.at[1:3, g], xr.at[g])

    def fresh(s):
        return [(a, b) for a, b in order if spans[s][0] <= order[a, b] < sum(spans[s])]

    def tile(t, s):
        top = STAGES[s][1]
        left = panel[0, 0:top].reshape(top * wide, quarter)
        right = panel[t, 0:top].reshape(top * wide, quarter)
        prod = contract(left, right)
        for a, b in fresh(s):
            x = fold(prod[a * wide:(a + 1) * wide, b * wide:(b + 1) * wide])
            x = x.reshape(2, 2, size, wide)
            for h in (0, 1):
                acc[t, h, order[a, b]] = x[:, h].reshape(2 * size, wide)
        send(acc.at[t, 1 - d, span(s)], take.at[t, span(s)], ds, dr.at[t, s], peer).start()

    def shared(s):
        top, half = STAGES[s][1], wide // 2
        for j in (1, 2):
            left = panel[j, 0:top, :, j - 1].reshape(top * half, quarter)
            right = panel[3 - j, 0:top].reshape(top * wide, quarter)
            prod = contract(left, right)
            for a, b in fresh(s):
                x = fold(prod[a * half:(a + 1) * half, b * wide:(b + 1) * wide])
                for h in (0, 1):
                    pacc[h, j - 1, order[a, b]] = x[h * size:(h + 1) * size]
            if s == last:
                for h in (0, 1):
                    dev = (flip(r, jnp.int32(j)), c, jnp.int32(h))
                    send(pacc.at[h, j - 1, span(s)], cross.at[j - 1, d], fs, fr, dev).start()
        if s < last:
            send(pacc.at[1 - d, :, span(s)], ptake.at[:, span(s)], ps, pr.at[s], peer).start()

    def settle(t, s):
        flush(take.at[t, span(s)], dr.at[t, s])
        acc[t, d, span(s)] += take[t, span(s)]

    def swap(s):
        flush(ptake.at[:, span(s)], pr.at[s])
        pacc[d, :, span(s)] += ptake[:, span(s)]
        for j in (1, 2):
            dst = acc.at[3, d, span(s), pl.ds((j - 1) * size, size)]
            send(pacc.at[d, j - 1, span(s)], dst, rs, rr.at[s], xdev[j]).start()

    def swapped(s):
        if s < last:
            flush(acc.at[3, d, span(s)], rr.at[s])
        else:
            flush(cross, fr)
            for j in (0, 1):
                acc[3, d, span(s), pl.ds(j * size, size)] = cross[j, 0] + cross[j, 1]

    def route(t):
        to = flip(r, jnp.asarray(t, jnp.int32))
        return to, lax.div(to, 2) != lax.div(c, 2)

    def chunk(n):
        s, skip, count = PIECES[n]
        return pl.ds(spans[s][0] + skip, count)

    def far(t, s, side=True):
        to, across = route(t)

        @pl.when(jnp.logical_and(jnp.logical_and(across, jnp.logical_not(inner)), side))
        def _():
            for n in range(len(PIECES)):
                if PIECES[n][0] == s:
                    send(acc.at[t, d, chunk(n)], relay.at[t, chunk(n)], gs, qr.at[t, n], zdev[1]).start()

    def near(t, s, side=True):
        to, across = route(t)

        @pl.when(jnp.logical_and(jnp.logical_and(to != c, jnp.logical_not(across)), side))
        def _():
            send(acc.at[t, d, span(s)], land.at[0, span(s)], gs, gr, zdev[1]).start()

    def pass_on(t, n, side=True):
        to, across = route(t)

        @pl.when(jnp.logical_and(jnp.logical_and(across, inner), side))
        def _():
            flush(relay.at[t, chunk(n)], qr.at[t, n])
            acc[t, d, chunk(n)] += relay[t, chunk(n)]
            send(acc.at[t, d, chunk(n)], land.at[1, chunk(n)], gs, gr, (r, to, d)).start()

    deep, edge_chip = inner, jnp.logical_not(inner)
    first = jnp.where(lax.div(r, 2) == lax.div(c, 2), 2, 1)
    second = 3 - first

    def operator():
        load_pot.wait()
        edge.wait()
        stencil(orb, halo, pot, applied)
        flush(panel.at[0, 0], ls)

    operator()
    forwards(((1, 0), (3, 0), (2, 0), (1, 1), (2, 1), (1, 2), (2, 2)), ((1, 0), (3, 0), (2, 0), (3, 1), (1, 1), (3, 2)))
    tile(0, 0)
    forwards(((1, 3), (2, 3)), ((1, 2), (1, 3), (1, 4)))
    settle(0, 0)
    far(0, 0)
    near(0, 0)
    gathered(0)
    gathered(1)
    shared(0)
    forwards(((1, 4), (2, 4)), ((3, 3), (3, 4)))
    tile(first, 0)
    forwards((), ((2, 1),))
    tile(second, 0)
    forwards(((3, 1),), ())
    swap(0)
    settle(first, 0)
    far(first, 0)
    settle(second, 0)
    far(second, 0)
    near(2, 0)
    near(1, 0)
    tile(0, 1)
    forwards(((3, 2),), ((2, 2),))
    settle(0, 1)
    far(0, 1)
    near(0, 1)
    forwards(((3, 3),), ((2, 3),))
    pass_on(0, 0)
    gathered(2)
    pass_on(first, 0)
    shared(1)
    forwards(((3, 4),), ((2, 4),))
    swapped(0)
    far(3, 0)
    near(3, 0)
    tile(first, 1)
    pass_on(second, 0)
    tile(second, 1)
    swap(1)
    settle(first, 1)
    far(first, 1)
    pass_on(3, 0)
    pass_on(0, 1)
    tile(0, 2)
    settle(second, 1)
    far(second, 1)
    near(2, 1, deep)
    near(1, 1, deep)
    gathered(3)
    shared(2)
    settle(0, 2)
    far(0, 2)
    near(0, 2, deep)
    swapped(1)
    far(3, 1)
    near(3, 1, deep)
    tile(first, 2)
    pass_on(first, 1)
    tile(second, 2)
    pass_on(second, 1)
    settle(first, 2)
    far(first, 2)
    near(2, 2, jnp.logical_and(deep, first == 2))
    near(1, 2, jnp.logical_and(deep, first == 1))
    settle(second, 2)
    far(second, 2)
    near(2, 2, jnp.logical_and(deep, first == 1))
    near(1, 2, jnp.logical_and(deep, first == 2))
    pass_on(3, 1)
    near(3, 1, edge_chip)
    near(2, 1, edge_chip)
    near(2, 2, edge_chip)
    pass_on(0, 2)
    pass_on(0, 3)
    swapped(2)
    far(3, 2)
    near(3, 2)
    near(1, 1, edge_chip)
    near(0, 2, edge_chip)
    near(1, 2, edge_chip)
    pass_on(first, 2)
    pass_on(first, 3)
    pass_on(3, 2)
    pass_on(3, 3)
    pass_on(second, 2)
    pass_on(second, 3)

    flush(panel.at[0, 0:3], zs)
    flush(panel.at[0:2], xs)
    flush(take, ds)
    flush(acc.at[3, 0, 0:spans[last][0]], rs)
    flush(ptake, ps)
    flush(cross, fs)
    mine = flip(r, c)
    flush(land, gr)
    acc[mine, d] = (acc[mine, d] + land[0] + land[1]) * dvol
    half, quad = wide // 2, wide // 8
    pick = lax.div(lane, quad)
    for a in range(GROUPS):
        for u, (kind, m) in enumerate(MEMBERS[a]):
            total = []
            for b in range(GROUPS):
                i, rows = order[a, b], pl.ds(u * size, size)
                total.append(acc[mine, d, i, rows])
            first = (d if kind == OUTER else 1 - d) * half + m * size
            for part in range(parts):
                for v in (0, 1):
                    out = None
                    for b in range(GROUPS):
                        for w, (col, n) in enumerate(MEMBERS[b]):
                            at = part * half + w * 2 * quad + v * quad
                            to = (col ^ v) * half + n * quad
                            moved = pltpu.roll(total[b], (to - at) % wide, 1)
                            out = moved if out is None else jnp.where(pick == to // quad, moved, out)
                    rows = pl.ds(pl.multiple_of(first, size), size)
                    inter[rows, part, pl.ds(v * wide, wide)] = out

    flush(relay.at[0:3], gs)


def publish(inter, applied, inter_out, applied_out, sems):
    copies = [
        pltpu.make_async_copy(applied, applied_out, sems.at[0]),
        pltpu.make_async_copy(inter, inter_out, sems.at[1]),
    ]
    for cp in copies:
        cp.start()
    for cp in copies:
        cp.wait()


def stay(array):
    return pltpu.with_memory_space_constraint(array, pltpu.HBM)


def exchange(orbitals, potential):
    parts, orbs, planes, cells = orbitals.shape
    rows = orbs * lax.axis_size("col")
    half = rows // 2
    size = orbs // GROUPS
    count = GROUPS * GROUPS
    steps, pieces = len(STAGES), len(PIECES)
    dvol = 1.0 / (planes * lax.axis_size("depth") * cells)
    vmem = pl.BlockSpec(memory_space=pltpu.VMEM)
    dma = pltpu.SemaphoreType.DMA
    block = (count, 2 * size, 8 * size)
    early = blocks()[1][-1][0]
    inter, applied = pl.pallas_call(
        functools.partial(kernel, dvol),
        out_shape=(
            jax.ShapeDtypeStruct((half, 2, rows), jnp.float32),
            jax.ShapeDtypeStruct((parts, orbs, cells), jnp.bfloat16),
        ),
        in_specs=[pl.BlockSpec(memory_space=pltpu.HBM)] * 2,
        out_specs=(vmem, vmem),
        scratch_shapes=[
            pltpu.VMEM((parts, orbs, cells), jnp.bfloat16),
            pltpu.VMEM(potential.shape, jnp.float32),
            pltpu.VMEM((parts, orbs, cells), jnp.bfloat16),
            pltpu.VMEM((3, GROUPS, parts, 2, 2, size, cells // 4), jnp.bfloat16),
            pltpu.VMEM((4, 2) + block, jnp.float32),
            pltpu.VMEM((3,) + block, jnp.float32),
            pltpu.VMEM((2, 2, count, size, 8 * size), jnp.float32),
            pltpu.VMEM((2, 2, count - early, size, 8 * size), jnp.float32),
            pltpu.VMEM((2,) + block, jnp.float32),
            pltpu.VMEM((4,) + block, jnp.float32),
            pltpu.VMEM((2, early, size, 8 * size), jnp.float32),
            dma((2,)), dma, dma, dma, dma, dma((4, len(CUTS))), dma, dma((GROUPS,)), dma, dma((3, steps)),
            dma, dma, dma((4, pieces)), dma, dma((steps,)), dma, dma((steps,)), dma, dma,
        ],
        compiler_params=pltpu.CompilerParams(
            collective_id=0, has_side_effects=True, vmem_limit_bytes=24000000
        ),
        name="overlap",
    )(stay(orbitals.reshape(parts, orbs, cells)), stay(potential))
    inter, applied = pl.pallas_call(
        publish,
        out_shape=(
            jax.ShapeDtypeStruct((half, 2, rows), jnp.float32),
            jax.ShapeDtypeStruct((parts, orbs, cells), jnp.bfloat16),
        ),
        in_specs=[vmem, vmem],
        out_specs=[pl.BlockSpec(memory_space=pltpu.HBM)] * 2,
        scratch_shapes=[dma((2,))],
        compiler_params=pltpu.CompilerParams(vmem_limit_bytes=16000000),
        name="publish",
    )(inter, applied)
    return inter, applied.reshape(orbitals.shape)


def solution(mesh):
    in_specs = (P(None, ("row", "col"), "depth", None), P("depth", None))
    out_specs = (P(("row", "depth"), None, "col"), P(None, ("row", "col"), "depth", None))
    sizes = tuple(mesh.shape[axis] for axis in ("row", "col", "depth"))
    body = exchange if sizes == (4, 4, 2) else shards
    return jax.shard_map(body, mesh=mesh, in_specs=in_specs, out_specs=out_specs, check_vma=False)
```

```python
import functools

import jax
import jax.numpy as jnp
from jax import lax
from jax.experimental import pallas as pl
from jax.experimental.pallas import tpu as pltpu
from jax.sharding import PartitionSpec as P

NX = 64
MESH = pl.DeviceIdType.MESH


def with_halo(block, sides, width):
    for axis, dim in sides:
        count = lax.axis_size(axis)
        forward = [(i, i + 1) for i in range(count - 1)]
        forward.append((count - 1, 0))
        backward = [(target, source) for source, target in forward]
        low = lax.ppermute(
            lax.slice_in_dim(block, block.shape[dim] - width, None, axis=dim), axis, forward
        )
        high = lax.ppermute(lax.slice_in_dim(block, 0, width, axis=dim), axis, backward)
        block = jnp.concatenate([low, block, high], axis=dim)
    return block


def apply_operator(padded, potential):
    center = padded[:, :, 1:-1].astype(jnp.float32)
    below = padded[:, :, :-2].astype(jnp.float32)
    above = padded[:, :, 2:].astype(jnp.float32)
    flat_cells = center.shape[-1]
    xpos = jnp.arange(flat_cells) % NX
    yminus = jnp.roll(center, NX, axis=3)
    yplus = jnp.roll(center, -NX, axis=3)
    xminus = jnp.where(xpos == 0, jnp.roll(center, 1 - NX, axis=3), jnp.roll(center, 1, axis=3))
    xplus = jnp.where(
        xpos == NX - 1, jnp.roll(center, NX - 1, axis=3), jnp.roll(center, -1, axis=3)
    )
    lap = below + above + yminus + yplus + xminus + xplus - 6.0 * center
    return (-0.5 * lap + potential[None, None] * center).astype(jnp.bfloat16)


def contract(left, right):
    return lax.dot_general(
        left, right, (((1,), (1,)), ((), ())), preferred_element_type=jnp.float32
    )


def shards(orbitals, potential):
    parts, orbs, planes, cells = orbitals.shape
    flat = orbitals.reshape(parts, orbs, planes * cells)
    panel = lax.all_gather(flat, "col", axis=1, tiled=True)
    other = lax.all_gather(flat, "row", axis=1, tiled=True)
    padded = with_halo(orbitals, (("depth", 2),), 1)
    applied = apply_operator(padded, potential)
    dvol = 1.0 / (planes * lax.axis_size("depth") * cells)
    tile_cols = other.shape[1]
    real_rows = panel[0]
    imag_rows = panel[1]
    sreal = contract(real_rows, other[0]) + contract(imag_rows, other[1])
    simag = contract(real_rows, other[1]) - contract(imag_rows, other[0])
    summed = lax.psum_scatter(
        dvol * jnp.concatenate([sreal, simag], axis=1), "depth", scatter_dimension=0, tiled=True
    )
    intersection = summed.reshape(summed.shape[0], 2, tile_cols)
    intersection = lax.all_to_all(intersection, "col", split_axis=2, concat_axis=2, tiled=True)
    return (intersection, applied)


def flip(a, b):
    low = lax.rem(lax.rem(a, 2) + lax.rem(b, 2), 2)
    high = lax.rem(lax.div(a, 2) + lax.div(b, 2), 2)
    return 2 * high + low


def stencil(orb, halo, pot, out):
    parts, orbs, cells = orb.shape
    step = 16
    xpos = lax.broadcasted_iota(jnp.int32, (step, cells), 1) % NX
    first, last = xpos == 0, xpos == NX - 1

    def body(i, carry):
        part = lax.div(i, orbs // step)
        rows = pl.ds(pl.multiple_of(lax.rem(i, orbs // step) * step, step), step)
        center = orb[part, rows, :].astype(jnp.float32)
        side = halo[part, rows, :].astype(jnp.float32)
        right = pltpu.roll(center, 1, 1)
        left = pltpu.roll(center, cells - 1, 1)
        yminus = pltpu.roll(center, NX, 1)
        yplus = pltpu.roll(center, cells - NX, 1)
        xminus = jnp.where(first, pltpu.roll(right, cells - NX, 1), right)
        xplus = jnp.where(last, pltpu.roll(left, NX, 1), left)
        lap = side + side + yminus + yplus + xminus + xplus - 6.0 * center
        out[part, rows, :] = (-0.5 * lap + pot[0:1, :] * center).astype(out.dtype)
        return carry

    lax.fori_loop(0, parts * (orbs // step), body, 0)


STAGES = ((0, 2), (2, 3), (3, 4))
PIECES = ((0, 0, 4), (1, 0, 5), (2, 0, 3), (2, 3, 2), (2, 5, 2))
GROUPS = 4
OUTER, INNER = 0, 1
MEMBERS = (
    ((OUTER, 0), (OUTER, 1)),
    ((OUTER, 2), (INNER, 0)),
    ((OUTER, 3), (INNER, 1)),
    ((INNER, 2), (INNER, 3)),
)
CUTS = ((0, 0, 2), (1, 0, 2), (2, 0, 2), (3, 0, 1), (3, 1, 1))
PLACE = {member: (g, u) for g, pair in enumerate(MEMBERS) for u, member in enumerate(pair)}


def blocks():
    order, spans = {}, []
    for low, high in STAGES:
        begin = len(order)
        for a in range(high):
            for b in range(high):
                if max(a, b) >= low:
                    order[a, b] = len(order)
        spans.append((begin, len(order) - begin))
    return order, spans


def kernel(dvol, orb_hbm, pot_hbm, inter, applied, orb, pot, halo, panel, acc, take, pacc, cross,
           land, relay, ptake, wire, ins, hs, hr, ls, zs, zr, xs, xr, ds, dr, gs, gr, qr, rs, rr, ps, pr, fs, fr):
    r, c, d = lax.axis_index("row"), lax.axis_index("col"), lax.axis_index("depth")
    parts, orbs, cells = orb.shape
    quarter = cells // 4
    size = orbs // GROUPS
    wide = 8 * size
    order, spans = blocks()
    load = pltpu.make_async_copy(orb_hbm, orb, ins.at[0])
    load.start()
    load_pot = pltpu.make_async_copy(pot_hbm, pot, ins.at[1])
    load_pot.start()
    peer = (r, c, 1 - d)
    zdev = [None] + [(r, flip(c, k), d) for k in (1, 2, 3)]
    xdev = [None] + [(flip(r, k), c, d) for k in (1, 2)]

    barrier = pltpu.get_barrier_semaphore()
    friends = [peer] + zdev[1:] + xdev[1:] + [(flip(r, k), c, 1 - d) for k in (1, 2)]
    for dev in friends:
        pl.semaphore_signal(barrier, inc=1, device_id=dev, device_id_type=MESH)
    load.wait()
    pl.semaphore_wait(barrier, len(friends))

    def send(src, dst, ssem, rsem, dev):
        return pltpu.make_async_remote_copy(
            src_ref=src, dst_ref=dst, send_sem=ssem, recv_sem=rsem,
            device_id=dev, device_id_type=MESH,
        )

    def own(m, k, begin=0, count=2):
        half = quarter // 2
        lanes = pl.ds(pl.multiple_of(k * quarter + begin * half, half), count * half)
        return orb.at[:, pl.ds(m * size, size), lanes]

    def place(m, k):
        deep = lax.rem(k + 1, 4) >= 2
        return [jnp.where(deep, i, o) for i, o in zip(PLACE[INNER, m], PLACE[OUTER, m])]

    def home(m, k):
        return place(m, k)[0]

    def spot(j, m, k, begin=0, count=2):
        g, u = place(m, k)
        half = quarter // 2
        return panel.at[j, g, :, u, lax.div(k, 2), :, pl.ds(begin * half, count * half)]

    def go(cp):
        cp.start()
        return cp

    def flush(ref, sem):
        pltpu.make_async_copy(ref, ref, sem).wait()

    zsend = {}
    for n, (m, *cut) in enumerate(CUTS):
        for k in (1, 3, 2):
            zsend[k, n] = go(send(own(m, flip(c, k), *cut), spot(0, m, c, *cut), zs, zr.at[k, n], zdev[k]))
    for g in range(GROUPS):
        for j in (1, 2):
            send(own(g, c), spot(j, g, c), xs, xr.at[home(g, c)], xdev[j]).start()
    edge = send(orb, halo, hs, hr, peer)
    edge.start()
    for g in range(GROUPS):
        pltpu.make_async_copy(own(g, c), spot(0, g, c), ls).start()

    inner = lax.rem(c + 1, 4) >= 2
    lane = lax.broadcasted_iota(jnp.int32, (1, 2 * wide // 2), 1)
    sign = jnp.where(lane < wide // 2, 1.0, -1.0).astype(jnp.float32)

    def fold(x):
        rows = x.shape[0] // 2
        return x[:rows] + sign * pltpu.roll(x[rows:], wide // 2, 1)

    def span(s):
        begin, count = spans[s]
        return pl.ds(begin, count)

    def forward(k, n):
        zsend[k, n].wait_recv()
        m, *cut = CUTS[n]
        for j in (1, 2):
            part = [spot(i, m, flip(c, k), *cut) for i in (0, j)]
            send(*part, xs, xr.at[home(m, flip(c, k))], xdev[j]).start()

    def forwards(deep, shallow):
        @pl.when(inner)
        def _():
            for k, m in deep:
                forward(k, m)

        @pl.when(jnp.logical_not(inner))
        def _():
            for k, m in shallow:
                forward(k, m)

    last = len(STAGES) - 1

    def gathered(g):
        flush(panel.at[1:3, g], xr.at[g])

    def fresh(s):
        return [(a, b) for a, b in order if spans[s][0] <= order[a, b] < sum(spans[s])]

    def tile(t, s):
        top = STAGES[s][1]
        left = panel[0, 0:top].reshape(top * wide, quarter)
        right = panel[t, 0:top].reshape(top * wide, quarter)
        prod = contract(left, right)
        for a, b in fresh(s):
            x = fold(prod[a * wide:(a + 1) * wide, b * wide:(b + 1) * wide])
            x = x.reshape(2, 2, size, wide)
            for h in (0, 1):
                acc[t, h, order[a, b]] = x[:, h].reshape(2 * size, wide)
        send(acc.at[t, 1 - d, span(s)], take.at[t, span(s)], ds, dr.at[t, s], peer).start()

    def shared(s):
        top, half = STAGES[s][1], wide // 2
        for j in (1, 2):
            left = panel[j, 0:top, :, j - 1].reshape(top * half, quarter)
            right = panel[3 - j, 0:top].reshape(top * wide, quarter)
            prod = contract(left, right)
            for a, b in fresh(s):
                x = fold(prod[a * half:(a + 1) * half, b * wide:(b + 1) * wide])
                for h in (0, 1):
                    pacc[h, j - 1, order[a, b]] = x[h * size:(h + 1) * size]
            if s == last:
                for h in (0, 1):
                    dev = (flip(r, jnp.int32(j)), c, jnp.int32(h))
                    send(pacc.at[h, j - 1, span(s)], cross.at[j - 1, d], fs, fr, dev).start()
        if s < last:
            send(pacc.at[1 - d, :, span(s)], ptake.at[:, span(s)], ps, pr.at[s], peer).start()

    def settle(t, s):
        flush(take.at[t, span(s)], dr.at[t, s])
        acc[t, d, span(s)] += take[t, span(s)]

    def swap(s):
        flush(ptake.at[:, span(s)], pr.at[s])
        pacc[d, :, span(s)] += ptake[:, span(s)]
        for j in (1, 2):
            dst = acc.at[3, d, span(s), pl.ds((j - 1) * size, size)]
            send(pacc.at[d, j - 1, span(s)], dst, rs, rr.at[s], xdev[j]).start()

    def swapped(s, side=True):
        if s < last:
            @pl.when(side)
            def _():
                flush(acc.at[3, d, span(s)], rr.at[s])
        else:
            flush(cross, fr)
            for j in (0, 1):
                acc[3, d, span(s), pl.ds(j * size, size)] = cross[j, 0] + cross[j, 1]

    def encode(t, blocks):
        x = acc[t, d, blocks]
        high = x.astype(jnp.bfloat16)
        base = high.astype(jnp.float32)
        steps = jnp.round((x - base) / jnp.maximum(jnp.abs(base), 1e-37) * 2048.0)
        steps = jnp.clip(steps, -7.0, 7.0)
        wire[t, blocks, :2 * size] = high
        wire[t, blocks, 2 * size:] = (steps[:, :size] * 16.0 + steps[:, size:]).astype(jnp.bfloat16)

    def decode(words):
        base = words[:, :2 * size].astype(jnp.float32)
        code = words[:, 2 * size:].astype(jnp.float32)
        upper = jnp.round(code / 16.0)
        steps = jnp.concatenate([upper, code - 16.0 * upper], axis=1)
        return base + steps * jnp.abs(base) / 2048.0

    def route(t):
        to = flip(r, jnp.asarray(t, jnp.int32))
        return to, lax.div(to, 2) != lax.div(c, 2)

    def chunk(n):
        s, skip, count = PIECES[n]
        return pl.ds(spans[s][0] + skip, count)

    def far(t, s, side=True):
        to, across = route(t)

        @pl.when(jnp.logical_and(jnp.logical_and(across, jnp.logical_not(inner)), side))
        def _():
            for n in range(len(PIECES)):
                if PIECES[n][0] == s:
                    encode(t, chunk(n))
                    send(wire.at[t, chunk(n)], relay.at[t, chunk(n)], gs, qr.at[t, n], zdev[1]).start()

    def near(t, s, side=True):
        to, across = route(t)

        @pl.when(jnp.logical_and(jnp.logical_and(to != c, jnp.logical_not(across)), side))
        def _():
            encode(t, span(s))
            send(wire.at[t, span(s)], land.at[0, span(s)], gs, gr, zdev[1]).start()

    def pass_on(t, n, side=True):
        to, across = route(t)

        @pl.when(jnp.logical_and(jnp.logical_and(across, inner), side))
        def _():
            flush(relay.at[t, chunk(n)], qr.at[t, n])
            acc[t, d, chunk(n)] += decode(relay[t, chunk(n)])
            encode(t, chunk(n))
            send(wire.at[t, chunk(n)], land.at[1, chunk(n)], gs, gr, (r, to, d)).start()

    deep, edge_chip = inner, jnp.logical_not(inner)
    first = jnp.where(lax.div(r, 2) == lax.div(c, 2), 2, 1)
    second = 3 - first

    def operator():
        load_pot.wait()
        edge.wait()
        stencil(orb, halo, pot, applied)
        flush(panel.at[0, 0], ls)

    operator()
    forwards(((1, 0), (3, 0), (2, 0), (1, 1), (2, 1), (1, 2), (2, 2)), ((1, 0), (3, 0), (2, 0), (3, 1), (1, 1), (3, 2)))
    tile(0, 0)
    forwards(((1, 3), (2, 3)), ((1, 2), (1, 3), (1, 4)))
    settle(0, 0)
    far(0, 0)
    near(0, 0)
    gathered(0)
    gathered(1)
    shared(0)
    forwards(((1, 4), (2, 4)), ((3, 3), (3, 4)))
    tile(first, 0)
    forwards((), ((2, 1),))
    tile(second, 0)
    forwards(((3, 1),), ())
    swap(0)
    settle(first, 0)
    far(first, 0)
    settle(second, 0)
    far(second, 0)
    near(2, 0)
    near(1, 0)
    tile(0, 1)
    forwards(((3, 2),), ((2, 2),))
    settle(0, 1)
    far(0, 1)
    near(0, 1)
    forwards(((3, 3),), ((2, 3),))
    pass_on(0, 0)
    gathered(2)
    pass_on(first, 0)
    shared(1)
    forwards(((3, 4),), ((2, 4),))
    swapped(0)
    far(3, 0)
    near(3, 0)
    tile(first, 1)
    pass_on(second, 0)
    tile(second, 1)
    swap(1)
    settle(first, 1)
    far(first, 1)
    pass_on(3, 0)
    pass_on(0, 1)
    tile(0, 2)
    settle(second, 1)
    far(second, 1)
    near(2, 1, deep)
    near(1, 1, deep)
    gathered(3)
    shared(2)
    settle(0, 2)
    far(0, 2)
    near(0, 2, deep)
    swapped(1, first == 2)
    far(3, 1)
    near(3, 1, jnp.logical_and(deep, first == 2))
    tile(first, 2)
    swapped(1, first == 1)
    near(3, 1, jnp.logical_and(deep, first == 1))
    pass_on(first, 1)
    tile(second, 2)
    pass_on(second, 1)
    settle(first, 2)
    far(first, 2)
    near(2, 2, jnp.logical_and(deep, first == 2))
    near(1, 2, jnp.logical_and(deep, first == 1))
    settle(second, 2)
    far(second, 2)
    near(2, 2, jnp.logical_and(deep, first == 1))
    near(1, 2, jnp.logical_and(deep, first == 2))
    pass_on(3, 1)
    near(3, 1, edge_chip)
    near(2, 1, edge_chip)
    near(2, 2, edge_chip)
    for n in (2, 3, 4):
        pass_on(0, n)
    swapped(2)
    far(3, 2)
    near(3, 2)
    near(1, 1, edge_chip)
    near(0, 2, edge_chip)
    near(1, 2, edge_chip)
    for n in (2, 3, 4):
        pass_on(first, n)
    for n in (2, 3, 4):
        pass_on(3, n)
    for n in (2, 3, 4):
        pass_on(second, n)

    flush(panel.at[0, 0:3], zs)
    flush(panel.at[0:2], xs)
    flush(take, ds)
    flush(acc.at[3, 0, 0:spans[last][0]], rs)
    flush(ptake, ps)
    flush(cross, fs)
    mine = flip(r, c)
    flush(land, gr)
    acc[mine, d] = (acc[mine, d] + decode(land[0]) + decode(land[1])) * dvol
    half, quad = wide // 2, wide // 8
    pick = lax.div(lane, quad)
    for a in range(GROUPS):
        for u, (kind, m) in enumerate(MEMBERS[a]):
            total = []
            for b in range(GROUPS):
                i, rows = order[a, b], pl.ds(u * size, size)
                total.append(acc[mine, d, i, rows])
            first = (d if kind == OUTER else 1 - d) * half + m * size
            for part in range(parts):
                for v in (0, 1):
                    out = None
                    for b in range(GROUPS):
                        for w, (col, n) in enumerate(MEMBERS[b]):
                            at = part * half + w * 2 * quad + v * quad
                            to = (col ^ v) * half + n * quad
                            moved = pltpu.roll(total[b], (to - at) % wide, 1)
                            out = moved if out is None else jnp.where(pick == to // quad, moved, out)
                    rows = pl.ds(pl.multiple_of(first, size), size)
                    inter[rows, part, pl.ds(v * wide, wide)] = out

    flush(relay.at[0:3], gs)


def publish(inter, applied, inter_out, applied_out, sems):
    copies = [
        pltpu.make_async_copy(applied, applied_out, sems.at[0]),
        pltpu.make_async_copy(inter, inter_out, sems.at[1]),
    ]
    for cp in copies:
        cp.start()
    for cp in copies:
        cp.wait()


def stay(array):
    return pltpu.with_memory_space_constraint(array, pltpu.HBM)


def exchange(orbitals, potential):
    parts, orbs, planes, cells = orbitals.shape
    rows = orbs * lax.axis_size("col")
    half = rows // 2
    size = orbs // GROUPS
    count = GROUPS * GROUPS
    steps, pieces = len(STAGES), len(PIECES)
    dvol = 1.0 / (planes * lax.axis_size("depth") * cells)
    vmem = pl.BlockSpec(memory_space=pltpu.VMEM)
    dma = pltpu.SemaphoreType.DMA
    block = (count, 2 * size, 8 * size)
    words = (count, 3 * size, 8 * size)
    early = blocks()[1][-1][0]
    inter, applied = pl.pallas_call(
        functools.partial(kernel, dvol),
        out_shape=(
            jax.ShapeDtypeStruct((half, 2, rows), jnp.float32),
            jax.ShapeDtypeStruct((parts, orbs, cells), jnp.bfloat16),
        ),
        in_specs=[pl.BlockSpec(memory_space=pltpu.HBM)] * 2,
        out_specs=(vmem, vmem),
        scratch_shapes=[
            pltpu.VMEM((parts, orbs, cells), jnp.bfloat16),
            pltpu.VMEM(potential.shape, jnp.float32),
            pltpu.VMEM((parts, orbs, cells), jnp.bfloat16),
            pltpu.VMEM((3, GROUPS, parts, 2, 2, size, cells // 4), jnp.bfloat16),
            pltpu.VMEM((4, 2) + block, jnp.float32),
            pltpu.VMEM((3,) + block, jnp.float32),
            pltpu.VMEM((2, 2, count, size, 8 * size), jnp.float32),
            pltpu.VMEM((2, 2, count - early, size, 8 * size), jnp.float32),
            pltpu.VMEM((2,) + words, jnp.bfloat16),
            pltpu.VMEM((4,) + words, jnp.bfloat16),
            pltpu.VMEM((2, early, size, 8 * size), jnp.float32),
            pltpu.VMEM((4,) + words, jnp.bfloat16),
            dma((2,)), dma, dma, dma, dma, dma((4, len(CUTS))), dma, dma((GROUPS,)), dma, dma((3, steps)),
            dma, dma, dma((4, pieces)), dma, dma((steps,)), dma, dma((steps,)), dma, dma,
        ],
        compiler_params=pltpu.CompilerParams(
            collective_id=0, has_side_effects=True, vmem_limit_bytes=24000000
        ),
        name="overlap",
    )(stay(orbitals.reshape(parts, orbs, cells)), stay(potential))
    inter, applied = pl.pallas_call(
        publish,
        out_shape=(
            jax.ShapeDtypeStruct((half, 2, rows), jnp.float32),
            jax.ShapeDtypeStruct((parts, orbs, cells), jnp.bfloat16),
        ),
        in_specs=[vmem, vmem],
        out_specs=[pl.BlockSpec(memory_space=pltpu.HBM)] * 2,
        scratch_shapes=[dma((2,))],
        compiler_params=pltpu.CompilerParams(vmem_limit_bytes=16000000),
        name="publish",
    )(inter, applied)
    return inter, applied.reshape(orbitals.shape)


def solution(mesh):
    in_specs = (P(None, ("row", "col"), "depth", None), P("depth", None))
    out_specs = (P(("row", "depth"), None, "col"), P(None, ("row", "col"), "depth", None))
    sizes = tuple(mesh.shape[axis] for axis in ("row", "col", "depth"))
    body = exchange if sizes == (4, 4, 2) else shards
    return jax.shard_map(body, mesh=mesh, in_specs=in_specs, out_specs=out_specs, check_vma=False)
```
